512 devices in a mesh: gx: 8 (over y), gy: 8 (over z), gz: 8 (over x, core).
Axes of the slice: x: 4, y: 8, z: 8, core: 2. Of those that a mesh axis runs over, the one named last changes fastest.
Arguments:
- source: float32 [2, 32, 64, 1024], P(None, 'gx', 'gy', 'gz'), may hold values from -6 to 6
- sigma_intra: float32 [3, 32, 64, 1024], P(None, 'gx', 'gy', 'gz'), may hold values from 0.3 to 3
- sigma_extra: float32 [3, 32, 64, 1024], P(None, 'gx', 'gy', 'gz'), may hold values from 0.5 to 3
- membrane: float32 [32, 64, 1024], P('gx', 'gy', 'gz'), may hold values from 0.5 to 5
Outputs:
- solution: float32 [2, 32, 64, 1024], P(None, 'gx', 'gy', 'gz')
- residual: float32 [2, 32, 64, 1024], P(None, 'gx', 'gy', 'gz')
The draws below stay inside these ranges and needn't reach their ends.
All inputs are finite; a program needn't handle non-finite values.
Results may differ from the reference program's by a relative error of at most 0.0009.
Values sent between devices are 32-bit elements; how exact they have to be, the bound alone decides.
A program may use at most 64 MiB of HBM per device.

```python
import math
import jax
import jax.numpy as jnp
from jax import lax

KRYLOV = 10
NX = 32
NY = 64
NZ = 1024


def steps_of(stream_key, shape, shards, low, largest):
    gain, own = 1.0, jax.random.fold_in(stream_key, 6)
    for dim, parts in shards:
        draws = jnp.exp(jax.random.uniform(jax.random.fold_in(own, dim), (parts,), jnp.float32, low / len(shards), largest / len(shards)))
        gain = gain * jnp.repeat(draws, shape[dim] // parts).reshape([-1 if axis == dim else 1 for axis in range(len(shape))])
    return gain


def normal_values(stream_key, shape, width, most, shards=(), dtype=jnp.bfloat16):
    array = jax.random.normal(stream_key, shape, jnp.float32) * width
    if len(shards) > 0:
        array = steps_of(stream_key, shape, shards, -0.22, 0.18) * array
    return jnp.clip(array, min=-most, max=most).astype(dtype)


def setup_inputs(seed: int = 0) -> dict:
    keys = jax.random.split(jax.random.key(seed), 5)
    return {
        "source": normal_values(keys[0], (2, NX, NY, NZ), 1.0, 6.0, ((1, 8), (2, 8), (3, 8)), jnp.float32),
        "sigma_intra": jnp.clip(jnp.exp(math.log(3.0) - 2.3025851 * jax.random.uniform(keys[1], (3, NX, NY, NZ), jnp.float32) ** steps_of(keys[1], (3, NX, NY, NZ), ((1, 8), (2, 8), (3, 8)), -0.2, 0.2)), 0.3, 3.0),
        "sigma_extra": jnp.clip(jnp.exp(math.log(3.0) - 1.7917595 * jax.random.uniform(keys[2], (3, NX, NY, NZ), jnp.float32) ** steps_of(keys[2], (3, NX, NY, NZ), ((1, 8), (2, 8), (3, 8)), -0.2, 0.2)), 0.5, 3.0),
        "membrane": jnp.clip(jnp.exp(math.log(5.0) - 2.3025851 * jax.random.uniform(keys[3], (NX, NY, NZ), jnp.float32) ** steps_of(keys[3], (NX, NY, NZ), ((0, 8), (1, 8), (2, 8)), -0.2, 0.2)), 0.5, 5.0),
    }


highest = lax.Precision.HIGHEST

def shifted(padded_grid, spatial, offset):
    pieces = [slice(1, -1), slice(1, -1), slice(1, -1)]
    if offset > 0:
        pieces[spatial] = slice(2, None)
    else:
        pieces[spatial] = slice(None, -2)
    return padded_grid[tuple(pieces)]

def face_terms(padded_sigma):
    upper_faces = []
    lower_faces = []
    for spatial in range(3):
        component = padded_sigma[spatial]
        middle = component[1:-1, 1:-1, 1:-1]
        upper_faces.append(0.5 * (middle + shifted(component, spatial, 1)))
        lower_faces.append(0.5 * (middle + shifted(component, spatial, -1)))
    diagonal = upper_faces[0] + lower_faces[0]
    for spatial in range(1, 3):
        diagonal = diagonal + upper_faces[spatial] + lower_faces[spatial]
    return (upper_faces, lower_faces, diagonal)

def apply_laplace(faces, padded_field):
    upper_faces, lower_faces, diagonal = faces
    result = diagonal * padded_field[1:-1, 1:-1, 1:-1]
    for spatial in range(3):
        result = result - upper_faces[spatial] * shifted(padded_field, spatial, 1)
        result = result - lower_faces[spatial] * shifted(padded_field, spatial, -1)
    return result

def operate(intra_faces, extra_faces, membrane, padded_pair):
    joined = padded_pair[0] + padded_pair[1]
    shared = apply_laplace(intra_faces, joined)
    leading = membrane * padded_pair[0, 1:-1, 1:-1, 1:-1] + shared
    second = shared + apply_laplace(extra_faces, padded_pair[1])
    return jnp.stack([leading, second])

def inverse_blocks(intra_faces, extra_faces, membrane):
    intra_sum = intra_faces[2]
    extra_sum = extra_faces[2]
    determinant = membrane * intra_sum + membrane * extra_sum + intra_sum * extra_sum
    return jnp.stack([(intra_sum + extra_sum) / determinant, -intra_sum / determinant, (membrane + intra_sum) / determinant])

def precondition(inverse, pair):
    leading = inverse[0] * pair[0] + inverse[1] * pair[1]
    second = inverse[1] * pair[0] + inverse[2] * pair[1]
    return jnp.stack([leading, second])

def least_squares(hessenberg, start_norm):
    krylov = hessenberg.shape[1]
    rotated = hessenberg
    target = jnp.zeros((krylov + 1,), jnp.float32).at[0].set(start_norm)
    for column in range(krylov):
        pivot = rotated[column, column]
        lower_entry = rotated[column + 1, column]
        radius = jnp.sqrt(pivot * pivot + lower_entry * lower_entry)
        cosine = pivot / radius
        sine_value = lower_entry / radius
        row_top = cosine * rotated[column] + sine_value * rotated[column + 1]
        row_below = -sine_value * rotated[column] + cosine * rotated[column + 1]
        rotated = rotated.at[column].set(row_top).at[column + 1].set(row_below)
        leading = cosine * target[column] + sine_value * target[column + 1]
        second = -sine_value * target[column] + cosine * target[column + 1]
        target = target.at[column].set(leading).at[column + 1].set(second)
    coeffs = jnp.zeros((krylov,), jnp.float32)
    for column in range(krylov - 1, -1, -1):
        partial_sum = jnp.sum(rotated[column, column + 1:] * coeffs[column + 1:])
        coeffs = coeffs.at[column].set((target[column] - partial_sum) / rotated[column, column])
    return coeffs

def reference(source, sigma_intra, sigma_extra, membrane):
    margins = ((0, 0), (1, 1), (1, 1), (1, 1))
    intra_faces = face_terms(jnp.pad(sigma_intra, margins))
    extra_faces = face_terms(jnp.pad(sigma_extra, margins))
    inverse = inverse_blocks(intra_faces, extra_faces, membrane)
    start_norm = jnp.sqrt(jnp.sum(source * source))
    basis = jnp.zeros((KRYLOV + 1,) + source.shape, jnp.float32).at[0].set(source / start_norm)
    hessenberg = jnp.zeros((KRYLOV + 1, KRYLOV), jnp.float32)
    for column in range(KRYLOV):
        solved = precondition(inverse, basis[column])
        applied = operate(intra_faces, extra_faces, membrane, jnp.pad(solved, margins))
        flat_basis = basis[:column + 1].reshape(column + 1, -1)
        project = jnp.dot(flat_basis, applied.reshape(-1), precision=highest)
        applied = applied - jnp.dot(project, flat_basis, precision=highest).reshape(applied.shape)
        new_norm = jnp.sqrt(jnp.sum(applied * applied))
        basis = basis.at[column + 1].set(applied / new_norm)
        hessenberg = hessenberg.at[:column + 1, column].set(project).at[column + 1, column].set(new_norm)
    coeffs = least_squares(hessenberg, start_norm)
    combined = jnp.dot(coeffs, basis[:KRYLOV].reshape(KRYLOV, -1), precision=highest).reshape(source.shape)
    solution = precondition(inverse, combined)
    remainder = jnp.zeros((KRYLOV + 1,), jnp.float32).at[0].set(start_norm) - jnp.dot(hessenberg, coeffs, precision=highest)
    residual = jnp.dot(remainder, basis.reshape(KRYLOV + 1, -1), precision=highest).reshape(source.shape)
    return (solution, residual)
```

```python
import functools

import jax
import jax.numpy as jnp
from jax import lax
from jax.experimental import pallas as pl
from jax.experimental.pallas import tpu as pltpu
from jax.sharding import PartitionSpec as P

KRYLOV = 10
AXES = ("gx", "gy", "gz")
MESH = pl.DeviceIdType.MESH
NX, NY, NZ = 4, 8, 128
Q = 2 * NX
PAIRS = (KRYLOV + 1) * (KRYLOV + 2) // 2
TILE = (NY, NZ)


def sublane():
    return lax.broadcasted_iota(jnp.int32, TILE, 0)


def lane():
    return lax.broadcasted_iota(jnp.int32, TILE, 1)


def cycle_kernel(
    sizes,
    source_hbm, intra_hbm, extra_hbm, membrane_hbm,
    solution_ref, residual_ref,
    sigma, member, basis, u,
    coef_x, coef_y, coef_z, edge_y, edge_z, block, inverse,
    sigma_gx, sigma_gy, sigma_gz,
    send_x, send_y, send_z, ghost_x, ghost_y, ghost_z,
    gram_rows, gram_all, mine, parts,
    local_sem, sigma_send, sigma_recv, send_sem, recv_sem, sum_send, sum_recv,
):
    where = [lax.axis_index(a) for a in AXES]
    has = [(where[d] > 0, where[d] < sizes[d] - 1) for d in range(3)]

    loads = [
        pltpu.make_async_copy(intra_hbm, sigma.at[0], local_sem.at[0]),
        pltpu.make_async_copy(extra_hbm, sigma.at[1], local_sem.at[1]),
        pltpu.make_async_copy(membrane_hbm, member, local_sem.at[2]),
        pltpu.make_async_copy(source_hbm, basis.at[0], local_sem.at[3]),
    ]
    for c in loads:
        c.start()

    for ref in (sigma_gx, sigma_gy, sigma_gz, ghost_x, ghost_y, ghost_z):
        ref[...] = jnp.zeros_like(ref)
    gram_all[...] = jnp.zeros_like(gram_all)

    barrier = pltpu.get_barrier_semaphore()
    for d in range(3):
        for j in range(1, sizes[d]):
            other = lax.rem(where[d] + j, sizes[d])
            pl.semaphore_signal(barrier, inc=1, device_id={AXES[d]: other}, device_id_type=MESH)
    for k in range(1, KRYLOV + 1):
        basis[k] = jnp.zeros_like(basis.at[k])
    for c in loads:
        c.wait()
    pl.semaphore_wait(barrier, sum(n - 1 for n in sizes))

    def remote(src, dst, ssem, rsem, d, side):
        step = 1 if side else -1
        return pltpu.make_async_remote_copy(
            src_ref=src, dst_ref=dst, send_sem=ssem, recv_sem=rsem,
            device_id={AXES[d]: where[d] + step}, device_id_type=MESH,
        )

    def sigma_copies(d, side):
        made = []
        for s in range(2):
            if d == 0:
                src, dst = sigma.at[s, 0, NX - 1 if side else 0], sigma_gx.at[1 - side, s]
            elif d == 1:
                row = NY - 1 if side else 0
                src, dst = sigma.at[s, 1, :, pl.ds(row, 1), :], sigma_gy.at[1 - side, s, :, pl.ds(0, 1), :]
            else:
                src, dst = sigma.at[s, 2], sigma_gz.at[1 - side, s]
            made.append(
                remote(src, dst, sigma_send.at[d, side, s], sigma_recv.at[d, 1 - side, s], d, side)
            )
        return made

    for d in range(3):
        for side in range(2):
            @pl.when(has[d][side])
            def _():
                for c in sigma_copies(d, side):
                    c.start()
    for d in range(3):
        for side in range(2):
            @pl.when(has[d][side])
            def _():
                for c in sigma_copies(d, side):
                    c.wait_send()
                for c in sigma_copies(d, 1 - side):
                    c.wait_recv()

    row, col = sublane(), lane()
    first_row, last_row = row == 0, row == NY - 1
    first_col, last_col = col == 0, col == NZ - 1
    diagonals = []
    for s in range(2):
        across = [sigma_gx[0, s]] + [sigma[s, 0, x] for x in range(NX)] + [sigma_gx[1, s]]
        total = []
        for x in range(NX):
            upper = 0.5 * (across[x + 1] + across[x + 2])
            lower = 0.5 * (across[x + 1] + across[x])
            coef_x[s, 0, x] = lower
            coef_x[s, 1, x] = upper
            diagonal = upper + lower
            here = sigma[s, 1, x]
            ahead = jnp.where(last_row, sigma_gy[1, s, x, 0:1, :], pltpu.roll(here, NY - 1, 0))
            behind = jnp.where(first_row, sigma_gy[0, s, x, 0:1, :], pltpu.roll(here, 1, 0))
            upper = 0.5 * (here + ahead)
            lower = 0.5 * (here + behind)
            coef_y[s, 0, x] = jnp.where(first_row, 0.0, lower)
            coef_y[s, 1, x] = jnp.where(last_row, 0.0, upper)
            edge_y[s, x] = jnp.where(first_row, lower, jnp.where(last_row, upper, 0.0))
            diagonal = diagonal + upper + lower
            here = sigma[s, 2, x]
            ahead = jnp.where(last_col, pltpu.roll(sigma_gz[1, s, x], NZ - 1, 1), pltpu.roll(here, NZ - 1, 1))
            behind = jnp.where(first_col, pltpu.roll(sigma_gz[0, s, x], 1, 1), pltpu.roll(here, 1, 1))
            upper = 0.5 * (here + ahead)
            lower = 0.5 * (here + behind)
            coef_z[s, 0, x] = jnp.where(first_col, 0.0, lower)
            coef_z[s, 1, x] = jnp.where(last_col, 0.0, upper)
            edge_z[s, x] = jnp.where(first_col, lower, jnp.where(last_col, upper, 0.0))
            total.append(diagonal + upper + lower)
        diagonals.append(total)
    for x in range(NX):
        di, de, m = diagonals[0][x], diagonals[1][x], member[x]
        det = m * di + m * de + di * de
        inverse[0, x] = (di + de) / det
        inverse[1, x] = -di / det
        inverse[2, x] = (m + di) / det
        block[0, x] = de / det
        block[1, x] = m / det

    def solved(v):
        joined, second = [], []
        for x in range(NX):
            a, b = v[x], v[NX + x]
            joined.append(block[0, x] * a + block[1, x] * b)
            second.append(inverse[1, x] * a + inverse[2, x] * b)
        return joined + second

    def stage(values):
        lo = values[0]
        hi = values[0]
        for q in range(Q):
            u[q] = values[q]
            send_y[0, pl.ds(q, 1), :] = values[q][0:1, :]
            send_y[1, pl.ds(q, 1), :] = values[q][NY - 1 : NY, :]
            low = pltpu.roll(values[q], 2 * q, 1) if q else values[q]
            high = pltpu.roll(values[q], 2 * q + 2, 1)
            lo = low if q == 0 else jnp.where(col == 2 * q, low, lo)
            hi = high if q == 0 else jnp.where(col == 2 * q + 1, high, hi)
        send_z[0] = lo
        send_z[1] = hi
        for s in range(2):
            send_x[0, s] = values[s * NX]
            send_x[1, s] = values[s * NX + NX - 1]

    def halo(slot, d, side):
        send = (send_x, send_y, send_z)[d]
        ghost = (ghost_x, ghost_y, ghost_z)[d]
        return remote(
            send.at[side], ghost.at[slot, 1 - side],
            send_sem.at[d, side], recv_sem.at[slot, d, 1 - side], d, side,
        )

    def start(slot):
        for d in (2, 0, 1):
            for side in range(2):
                @pl.when(has[d][side])
                def _():
                    halo(slot, d, side).start()

    def finish(slot):
        for d in (0, 1, 2):
            for side in range(2):
                @pl.when(has[d][side])
                def _():
                    halo(slot, d, side).wait_send()
                    halo(slot, d, 1 - side).wait_recv()

    def gram_row(k):
        at = [basis[k, q // NX, q % NX] for q in range(Q)]
        for i in range(KRYLOV + 1):
            total = at[0] * basis[i, 0, 0]
            for q in range(1, Q):
                total = total + at[q] * basis[i, q // NX, q % NX]
            gram_rows[k, pl.ds(i, 1), :] = jnp.sum(total, axis=0, keepdims=True)

    def inner(s, x):
        field = u[s * NX + x]
        r = coef_y[s, 0, x] * pltpu.roll(field, 1, 0) + coef_y[s, 1, x] * pltpu.roll(field, NY - 1, 0)
        r = r + coef_z[s, 0, x] * pltpu.roll(field, 1, 1) + coef_z[s, 1, x] * pltpu.roll(field, NZ - 1, 1)
        if x > 0:
            r = r + coef_x[s, 0, x] * u[s * NX + x - 1]
        if x < NX - 1:
            r = r + coef_x[s, 1, x] * u[s * NX + x + 1]
        return r

    def advance(k, slot, twice, previous):
        partial = [inner(s, x) for s in range(2) for x in range(NX)]
        gram_row(k)
        finish(slot)
        beside = jnp.where(lax.rem(col, 2) == 1, ghost_z[slot, 0], ghost_z[slot, 1])
        off = []
        for s in range(2):
            for x in range(NX):
                q = s * NX + x
                r = partial[q]
                if x == 0:
                    r = r + coef_x[s, 0, x] * ghost_x[slot, 0, s]
                if x == NX - 1:
                    r = r + coef_x[s, 1, x] * ghost_x[slot, 1, s]
                rows = jnp.where(row < NY // 2, ghost_y[slot, 0, pl.ds(q, 1), :], ghost_y[slot, 1, pl.ds(q, 1), :])
                r = r + edge_y[s, x] * rows
                r = r + edge_z[s, x] * pltpu.roll(beside, NZ - (2 * q + 1), 1)
                off.append(r)
        new = [off[x] for x in range(NX)] + [off[x] + off[NX + x] for x in range(NX)]
        if twice:
            new = [2.0 * new[q] - basis[previous, q // NX, q % NX] for q in range(Q)]
        return new

    def keep(k, v):
        for q in range(Q):
            basis[k, q // NX, q % NX] = v[q]

    stage(solved([basis[0, q // NX, q % NX] for q in range(Q)]))
    start(0)
    v = advance(0, 0, False, None)
    stage(solved(v))
    start(1)
    keep(1, v)

    def step(k, carry):
        slot = lax.rem(k, 2)
        v = advance(k, slot, True, k - 1)
        stage(solved(v))
        start(1 - slot)
        keep(k + 1, v)
        return carry

    lax.fori_loop(1, KRYLOV - 1, step, 0)
    keep(KRYLOV, advance(KRYLOV - 1, (KRYLOV - 1) % 2, True, KRYLOV - 2))
    gram_row(KRYLOV)

    at = 0
    for k in range(KRYLOV + 1):
        gram_all[pl.ds(at, k + 1), :] = gram_rows[k, pl.ds(0, k + 1), :]
        at += k + 1
    summed = lax.dot_general(
        jnp.ones(TILE, jnp.float32), gram_all[...], (((1,), (1,)), ((), ())),
        precision=lax.Precision.HIGHEST, preferred_element_type=jnp.float32,
    )
    for n, d in enumerate((2, 1, 0)):
        size = sizes[d]
        mine[n, 0:1, :] = summed[0:1, :]
        parts[n, where[d], 0:1, :] = summed[0:1, :]

        def copy(j):
            other = lax.rem(where[d] + j, size)
            return pltpu.make_async_remote_copy(
                src_ref=mine.at[n, pl.ds(0, 1), :], dst_ref=parts.at[n, where[d], pl.ds(0, 1), :],
                send_sem=sum_send.at[n, j], recv_sem=sum_recv.at[n, where[d]],
                device_id={AXES[d]: other}, device_id_type=MESH,
            )

        def arrival(j):
            other = lax.rem(where[d] + j, size)
            return pltpu.make_async_remote_copy(
                src_ref=mine.at[n, pl.ds(0, 1), :], dst_ref=parts.at[n, other, pl.ds(0, 1), :],
                send_sem=sum_send.at[n, j], recv_sem=sum_recv.at[n, other],
                device_id={AXES[d]: other}, device_id_type=MESH,
            )

        for j in range(1, size):
            copy(j).start()
        for j in range(1, size):
            arrival(j).wait_recv()
        for j in range(1, size):
            copy(j).wait_send()
        terms = [parts[n, j, 0:1, :] for j in range(size)]
        while len(terms) > 1:
            terms = [terms[i] + terms[i + 1] for i in range(0, len(terms), 2)]
        summed = terms[0]

    g = {}
    at = 0
    for k in range(KRYLOV + 1):
        for i in range(k + 1):
            g[k, i] = jnp.broadcast_to(summed[:, at : at + 1], TILE)
            at += 1
    size = KRYLOV + 1
    right = [jnp.ones(TILE, jnp.float32) for _ in range(size)]
    over = []
    for k in range(size):
        over.append(1.0 / g[k, k])
        for i in range(k + 1, size):
            factor = g[i, k] * over[k]
            for j in range(k + 1, i + 1):
                g[i, j] = g[i, j] - factor * g[j, k]
            right[i] = right[i] - factor * right[k]
    z = [None] * size
    for k in range(size - 1, -1, -1):
        rest = right[k]
        for j in range(k + 1, size):
            rest = rest - g[j, k] * z[j]
        z[k] = rest * over[k]
    total = z[0]
    for k in range(1, size):
        total = total + z[k]
    scale = 1.0 / total
    rho = [scale * a for a in z]
    tail, slope = [None] * size, [None] * size
    running = jnp.zeros(TILE, jnp.float32)
    weighted = jnp.zeros(TILE, jnp.float32)
    for j in range(KRYLOV - 1, -1, -1):
        running = running + rho[j + 1]
        weighted = weighted + running
        slope[j] = weighted
    coeffs = [slope[0]] + [2.0 * slope[j] for j in range(1, KRYLOV)]

    for x in range(NX):
        left, below = [], []
        for s in range(2):
            vectors = [basis[k, s, x] for k in range(size)]
            r = rho[0] * vectors[0]
            c = coeffs[0] * vectors[0]
            for k in range(1, size):
                r = r + rho[k] * vectors[k]
                if k < KRYLOV:
                    c = c + coeffs[k] * vectors[k]
            residual_ref[s, x] = r
            left.append(c)
        solution_ref[0, x] = inverse[0, x] * left[0] + inverse[1, x] * left[1]
        solution_ref[1, x] = inverse[1, x] * left[0] + inverse[2, x] * left[1]


def body(source, sigma_intra, sigma_extra, membrane):
    sizes = tuple(lax.axis_size(a) for a in AXES)
    f32 = jnp.float32
    vm = lambda *s: pltpu.VMEM(s, f32)
    dma = pltpu.SemaphoreType.DMA
    out = jax.ShapeDtypeStruct(source.shape, f32)
    return pl.pallas_call(
        functools.partial(cycle_kernel, sizes),
        out_shape=(out, out),
        in_specs=[pl.BlockSpec(memory_space=pl.ANY)] * 4,
        out_specs=(pl.BlockSpec(memory_space=pltpu.VMEM),) * 2,
        scratch_shapes=[
            vm(2, 3, NX, *TILE), vm(NX, *TILE), vm(KRYLOV + 1, 2, NX, *TILE), vm(Q, *TILE),
            vm(2, 2, NX, *TILE), vm(2, 2, NX, *TILE), vm(2, 2, NX, *TILE),
            vm(2, NX, *TILE), vm(2, NX, *TILE), vm(2, NX, *TILE), vm(3, NX, *TILE),
            vm(2, 2, *TILE), vm(2, 2, NX, *TILE), vm(2, 2, NX, *TILE),
            vm(2, 2, *TILE), vm(2, *TILE), vm(2, *TILE),
            vm(2, 2, 2, *TILE), vm(2, 2, *TILE), vm(2, 2, *TILE),
            vm(KRYLOV + 1, 16, NZ), vm(128, NZ), vm(3, *TILE), vm(3, 8, *TILE),
            dma((4,)), dma((3, 2, 2)), dma((3, 2, 2)), dma((3, 2)), dma((2, 3, 2)),
            dma((3, 8)), dma((3, 8)),
        ],
        compiler_params=pltpu.CompilerParams(collective_id=0, has_side_effects=True),
    )(source, sigma_intra, sigma_extra, membrane)


def solution(mesh):
    return jax.shard_map(
        body,
        mesh=mesh,
        in_specs=(
            P(None, "gx", "gy", "gz"),
            P(None, "gx", "gy", "gz"),
            P(None, "gx", "gy", "gz"),
            P("gx", "gy", "gz"),
        ),
        out_specs=(P(None, "gx", "gy", "gz"), P(None, "gx", "gy", "gz")),
        check_vma=False,
    )
```

```python
import functools
import itertools

import jax
import jax.numpy as jnp
from jax import lax
from jax.experimental import pallas as pl
from jax.experimental.pallas import tpu as pltpu
from jax.sharding import PartitionSpec as P

KRYLOV = 10
AXES = ("gx", "gy", "gz")
MESH = pl.DeviceIdType.MESH
NX, NY, NZ = 4, 8, 128
PAIRS = (KRYLOV + 1) * (KRYLOV + 2) // 2
TILE = (NY, NZ)
OWN, BESIDE = 0, 1
DIRECTIONS = [
    d for d in itertools.product((-1, 0, 1), repeat=3) if 1 <= sum(abs(a) for a in d) <= 2
]
TILES = (
    [(x, OWN, OWN) for x in range(-1, NX + 1)]
    + [(x, BESIDE, OWN) for x in range(NX)]
    + [(x, OWN, BESIDE) for x in range(NX)]
)
PLACE = {t: n for n, t in enumerate(TILES)}
FIELDS = 7


class Halo:
    def __init__(self, refs, fields, where, sizes):
        (self.own, self.pack, self.gx, self.gy, self.gz, self.gxy, self.gxz, self.gyz,
         self.send_sem, self.recv_sem) = refs
        self.fields, self.where, self.sizes = fields, where, sizes

    def exists(self, direction):
        there = None
        for axis, step in enumerate(direction):
            if step:
                at = self.where[axis]
                ok = at > 0 if step < 0 else at < self.sizes[axis] - 1
                there = ok if there is None else jnp.logical_and(there, ok)
        return there

    def copy(self, slot, direction):
        n = DIRECTIONS.index(direction)
        dx, dy, dz = direction
        ghost_x, ghost_z = (0 if dx > 0 else 1), (0 if dz > 0 else 1)
        row = NY - 1 if dy > 0 else 0
        if dx and dy:
            src = self.own.at[:, NX - 1 if dx > 0 else 0, pl.ds(row, 1), :]
            dst = self.gxy.at[slot, ghost_x, :, pl.ds(row, 1), :]
        elif dx and dz:
            src, dst = self.pack.at[...], self.gxz.at[slot, ghost_x, ghost_z]
        elif dy and dz:
            src = self.pack.at[pl.ds(row, 1), :]
            dst = self.gyz.at[slot, ghost_z, pl.ds(row, 1), :]
        elif dx:
            src = self.own.at[:, pl.ds(NX - 2 if dx > 0 else 0, 2)]
            dst = self.gx.at[slot, ghost_x]
        elif dy:
            rows = pl.ds(NY - 2 if dy > 0 else 0, 2)
            src, dst = self.own.at[:, :, rows, :], self.gy.at[slot, :, :, rows, :]
        else:
            src, dst = self.pack.at[...], self.gz.at[slot, ghost_z]
        return pltpu.make_async_remote_copy(
            src_ref=src, dst_ref=dst,
            send_sem=self.send_sem.at[n], recv_sem=self.recv_sem.at[slot, n],
            device_id={AXES[a]: self.where[a] + step for a, step in enumerate(direction) if step},
            device_id_type=MESH,
        )

    def fill_pack(self, values):
        group = lax.broadcasted_iota(jnp.int32, TILE, 1) // 4
        packed = None
        for q, v in enumerate(values):
            moved = pltpu.roll(v, 4 * q + 2, 1)
            packed = moved if packed is None else jnp.where(group == q, moved, packed)
        self.pack[...] = packed

    def start(self, slot):
        order = sorted(DIRECTIONS, key=lambda d: -sum(abs(a) for a in d))
        for d in order:
            @pl.when(self.exists(d))
            def _(d=d):
                self.copy(slot, d).start()

    def finish(self, slot):
        for d in DIRECTIONS:
            @pl.when(self.exists(d))
            def _(d=d):
                self.copy(slot, d).wait_send()
        order = sorted(DIRECTIONS, key=lambda d: sum(abs(a) for a in d))
        for d in order:
            @pl.when(self.exists(tuple(-a for a in d)))
            def _(d=d):
                self.copy(slot, d).wait_recv()

    def view(self, slot):
        return View(self, slot)


class View:
    def __init__(self, halo, slot):
        pair = lax.broadcasted_iota(jnp.int32, TILE, 1) % 4 < 2
        self.halo, self.slot, self.made = halo, slot, {}
        merge = lambda ref, *at: jnp.where(pair, ref[(slot, *at, 0)], ref[(slot, *at, 1)])
        self.wz = merge(halo.gz)
        self.wx = [merge(halo.gxz, 0), merge(halo.gxz, 1)]
        self.wy = merge(halo.gyz)

    def tile(self, f, x, ty, tz, turn=0):
        key = (f, x, ty, tz, turn)
        if key not in self.made:
            self.made[key] = self.make(f, x, ty, tz, turn)
        return self.made[key]

    def make(self, f, x, ty, tz, turn):
        h = self.halo
        if tz == BESIDE:
            if ty == BESIDE:
                source, plane = self.wy, x
            elif x < 0:
                source, plane = self.wx[0], NX - 1
            elif x >= NX:
                source, plane = self.wx[1], 0
            else:
                source, plane = self.wz, x
            return pltpu.roll(source, (NZ - (4 * (f * NX + plane) + 2) + turn) % NZ, 1)
        if turn:
            return pltpu.roll(self.tile(f, x, ty, tz), turn % NZ, 1)
        if ty == BESIDE:
            if x < 0:
                return h.gxy[self.slot, 0, f]
            if x >= NX:
                return h.gxy[self.slot, 1, f]
            return h.gy[self.slot, f, x]
        if x < 0:
            return h.gx[self.slot, 0, f, x + 2]
        if x >= NX:
            return h.gx[self.slot, 1, f, x - NX]
        return h.own[f, x]


class Values:
    def __init__(self, values):
        self.values, self.made = values, {}

    def tile(self, f, x, ty, tz, turn=0):
        v = self.values[f][x, ty, tz]
        if not turn:
            return v
        key = (f, x, ty, tz, turn)
        if key not in self.made:
            self.made[key] = pltpu.roll(v, turn % NZ, 1)
        return self.made[key]


def beside(view, f, t, axis, step):
    x, ty, tz = t
    if axis == 0:
        return view.tile(f, x + step, ty, tz)
    if axis == 1:
        edge = lax.broadcasted_iota(jnp.int32, TILE, 0) == (0 if step < 0 else NY - 1)
        shift = 1 if step < 0 else NY - 1
        return jnp.where(
            edge,
            pltpu.roll(view.tile(f, x, 1 - ty, tz), shift, 0),
            pltpu.roll(view.tile(f, x, ty, tz), shift, 0),
        )
    edge = lax.broadcasted_iota(jnp.int32, TILE, 1) == (0 if step < 0 else NZ - 1)
    return jnp.where(edge, view.tile(f, x, ty, 1 - tz, -step), view.tile(f, x, ty, tz, -step))


def cycle_kernel(
    sizes,
    source_hbm, intra_hbm, extra_hbm, membrane_hbm,
    solution_ref, residual_ref,
    basis, coef, block, inverse,
    s_own, s_pack, s_gx, s_gy, s_gz, s_gxy, s_gxz, s_gyz, s_send, s_recv,
    u_own, u_pack, u_gx, u_gy, u_gz, u_gxy, u_gxz, u_gyz, u_send, u_recv,
    gram_rows, gram_all, mine, parts,
    local_sem, sum_send, sum_recv,
):
    where = [lax.axis_index(a) for a in AXES]
    cells = Halo(
        (s_own, s_pack, s_gx, s_gy, s_gz, s_gxy, s_gxz, s_gyz, s_send, s_recv), FIELDS, where, sizes
    )
    halo = Halo(
        (u_own, u_pack, u_gx, u_gy, u_gz, u_gxy, u_gxz, u_gyz, u_send, u_recv), 2, where, sizes
    )

    loads = [
        pltpu.make_async_copy(intra_hbm, s_own.at[pl.ds(0, 3)], local_sem.at[0]),
        pltpu.make_async_copy(extra_hbm, s_own.at[pl.ds(3, 3)], local_sem.at[1]),
        pltpu.make_async_copy(membrane_hbm, s_own.at[6], local_sem.at[2]),
        pltpu.make_async_copy(source_hbm, basis.at[0], local_sem.at[3]),
    ]
    for c in loads:
        c.start()
    for h in (cells, halo):
        for ref in (h.gx, h.gy, h.gz, h.gxy, h.gxz, h.gyz):
            ref[...] = jnp.zeros_like(ref)

    barrier = pltpu.get_barrier_semaphore()
    expected = 0
    for d in DIRECTIONS:
        there = cells.exists(d)
        expected = expected + jnp.where(there, 1, 0)

        @pl.when(there)
        def _(d=d):
            pl.semaphore_signal(
                barrier, inc=1,
                device_id={AXES[a]: where[a] + step for a, step in enumerate(d) if step},
                device_id_type=MESH,
            )
    for d in range(3):
        for j in range(1, sizes[d]):
            other = lax.rem(where[d] + j, sizes[d])
            pl.semaphore_signal(barrier, inc=1, device_id={AXES[d]: other}, device_id_type=MESH)
    gram_all[...] = jnp.zeros_like(gram_all)
    for k in range(1, KRYLOV + 1):
        basis[k] = jnp.zeros_like(basis.at[k])
    for c in loads:
        c.wait()
    cells.fill_pack([s_own[f, x] for f in range(FIELDS) for x in range(NX)])
    pl.semaphore_wait(barrier, expected + sum(n - 1 for n in sizes))

    cells.start(0)
    cells.finish(0)
    view = cells.view(0)
    for t in TILES:
        n = PLACE[t]
        diagonals = []
        for s in range(2):
            total = None
            for axis in range(3):
                here = view.tile(3 * s + axis, *t)
                lower = 0.5 * (here + beside(view, 3 * s + axis, t, axis, -1))
                upper = 0.5 * (here + beside(view, 3 * s + axis, t, axis, 1))
                coef[s, n, 2 * axis] = lower
                coef[s, n, 2 * axis + 1] = upper
                total = upper + lower if total is None else total + upper + lower
            diagonals.append(total)
        di, de, m = diagonals[0], diagonals[1], view.tile(6, *t)
        det = m * di + m * de + di * de
        inside = m > 0.0
        over = jnp.where(inside, 1.0 / jnp.where(inside, det, 1.0), 0.0)
        block[n, 0] = de * over
        block[n, 1] = m * over
        block[n, 2] = -di * over
        block[n, 3] = (m + di) * over
        if n in range(1, NX + 1):
            inverse[n - 1] = (di + de) * over

    def solved(t, a, b):
        n = PLACE[t]
        return block[n, 0] * a + block[n, 1] * b, block[n, 2] * a + block[n, 3] * b

    def apply(view, t):
        n = PLACE[t]
        off = []
        for s in range(2):
            total = None
            for axis in range(3):
                for side, step in enumerate((-1, 1)):
                    term = coef[s, n, 2 * axis + side] * beside(view, s, t, axis, step)
                    total = term if total is None else total + term
            off.append(total)
        return off[0], off[0] + off[1]

    own = [(x, OWN, OWN) for x in range(NX)]

    def load(k):
        return [[basis[k, s, x] for x in range(NX)] for s in range(2)]

    def keep(k, v):
        for s in range(2):
            for x in range(NX):
                basis[k, s, x] = v[s][x]

    def stage(v):
        values = [[None] * NX for _ in range(2)]
        for x in range(NX):
            values[0][x], values[1][x] = solved(own[x], v[0][x], v[1][x])
        for s in range(2):
            for x in range(NX):
                u_own[s, x] = values[s][x]
        halo.fill_pack(values[0] + values[1])

    def gram_row(k):
        at = load(k)
        for i in range(KRYLOV + 1):
            total = None
            for s in range(2):
                for x in range(NX):
                    term = at[s][x] * basis[i, s, x]
                    total = term if total is None else total + term
            gram_rows[k, pl.ds(i, 1), :] = jnp.sum(total, axis=0, keepdims=True)

    def two_steps(slot):
        view = halo.view(slot)
        first, next_u = {}, [{}, {}]
        for t in TILES:
            first[t] = apply(view, t)
            next_u[0][t], next_u[1][t] = solved(t, *first[t])
        values = Values(next_u)
        second = [apply(values, t) for t in own]
        return (
            [[first[t][s] for t in own] for s in range(2)],
            [[second[x][s] for x in range(NX)] for s in range(2)],
        )

    every = [(s, x) for s in range(2) for x in range(NX)]

    def combine(f, *vs):
        return [[f(*(v[s][x] for v in vs)) for x in range(NX)] for s in range(2)]

    def advance(k, slot):
        w, b = two_steps(slot)
        odd = combine(lambda p, q: 2.0 * p - q, w, load(k - 1))
        even = combine(lambda p, q, r: 4.0 * p - 2.0 * q - r, b, load(k), load(k - 2))
        return odd, even

    stage(load(0))
    halo.start(0)
    gram_row(0)
    halo.finish(0)
    odd, b = two_steps(0)
    even = combine(lambda p, q: 2.0 * p - q, b, load(0))
    stage(even)
    halo.start(1)
    keep(1, odd)
    keep(2, even)

    def step(r, carry):
        k, slot = 2 * r, lax.rem(r, 2)
        gram_row(k - 1)
        gram_row(k)
        halo.finish(slot)
        odd, even = advance(k, slot)
        stage(even)
        halo.start(1 - slot)
        keep(k + 1, odd)
        keep(k + 2, even)
        return carry

    rounds = KRYLOV // 2
    lax.fori_loop(1, rounds - 1, step, 0)
    gram_row(KRYLOV - 3)
    gram_row(KRYLOV - 2)
    last = (rounds - 1) % 2
    halo.finish(last)
    odd, even = advance(KRYLOV - 2, last)
    keep(KRYLOV - 1, odd)
    keep(KRYLOV, even)
    gram_row(KRYLOV - 1)
    gram_row(KRYLOV)

    at = 0
    for k in range(KRYLOV + 1):
        gram_all[pl.ds(at, k + 1), :] = gram_rows[k, pl.ds(0, k + 1), :]
        at += k + 1
    summed = lax.dot_general(
        jnp.ones(TILE, jnp.float32), gram_all[...], (((1,), (1,)), ((), ())),
        precision=lax.Precision.HIGHEST, preferred_element_type=jnp.float32,
    )
    for n, d in enumerate((2, 1, 0)):
        size = sizes[d]
        mine[n, 0:1, :] = summed[0:1, :]
        parts[n, where[d], 0:1, :] = summed[0:1, :]

        def copy(j):
            other = lax.rem(where[d] + j, size)
            return pltpu.make_async_remote_copy(
                src_ref=mine.at[n, pl.ds(0, 1), :], dst_ref=parts.at[n, where[d], pl.ds(0, 1), :],
                send_sem=sum_send.at[n, j], recv_sem=sum_recv.at[n, where[d]],
                device_id={AXES[d]: other}, device_id_type=MESH,
            )

        def arrival(j):
            other = lax.rem(where[d] + j, size)
            return pltpu.make_async_remote_copy(
                src_ref=mine.at[n, pl.ds(0, 1), :], dst_ref=parts.at[n, other, pl.ds(0, 1), :],
                send_sem=sum_send.at[n, j], recv_sem=sum_recv.at[n, other],
                device_id={AXES[d]: other}, device_id_type=MESH,
            )

        for j in range(1, size):
            copy(j).start()
        for j in range(1, size):
            arrival(j).wait_recv()
        for j in range(1, size):
            copy(j).wait_send()
        terms = [parts[n, j, 0:1, :] for j in range(size)]
        while len(terms) > 1:
            terms = [terms[i] + terms[i + 1] for i in range(0, len(terms), 2)]
        summed = terms[0]

    g = {}
    at = 0
    for k in range(KRYLOV + 1):
        for i in range(k + 1):
            g[k, i] = jnp.broadcast_to(summed[:, at : at + 1], TILE)
            at += 1
    size = KRYLOV + 1
    right = [jnp.ones(TILE, jnp.float32) for _ in range(size)]
    over = []
    for k in range(size):
        over.append(1.0 / g[k, k])
        for i in range(k + 1, size):
            factor = g[i, k] * over[k]
            for j in range(k + 1, i + 1):
                g[i, j] = g[i, j] - factor * g[j, k]
            right[i] = right[i] - factor * right[k]
    z = [None] * size
    for k in range(size - 1, -1, -1):
        rest = right[k]
        for j in range(k + 1, size):
            rest = rest - g[j, k] * z[j]
        z[k] = rest * over[k]
    total = z[0]
    for k in range(1, size):
        total = total + z[k]
    scale = 1.0 / total
    rho = [scale * a for a in z]
    slope = [None] * size
    running = jnp.zeros(TILE, jnp.float32)
    weighted = jnp.zeros(TILE, jnp.float32)
    for j in range(KRYLOV - 1, -1, -1):
        running = running + rho[j + 1]
        weighted = weighted + running
        slope[j] = weighted
    coeffs = [slope[0]] + [2.0 * slope[j] for j in range(1, KRYLOV)]

    for x in range(NX):
        combined = []
        for s in range(2):
            vectors = [basis[k, s, x] for k in range(size)]
            r = rho[0] * vectors[0]
            c = coeffs[0] * vectors[0]
            for k in range(1, size):
                r = r + rho[k] * vectors[k]
                if k < KRYLOV:
                    c = c + coeffs[k] * vectors[k]
            residual_ref[s, x] = r
            combined.append(c)
        n = PLACE[own[x]]
        solution_ref[0, x] = inverse[x] * combined[0] + block[n, 2] * combined[1]
        solution_ref[1, x] = block[n, 2] * combined[0] + block[n, 3] * combined[1]


def halo_scratch(fields, slots):
    vm = lambda *s: pltpu.VMEM(s, jnp.float32)
    dma = pltpu.SemaphoreType.DMA
    count = len(DIRECTIONS)
    return [
        vm(fields, NX, *TILE), vm(*TILE),
        vm(slots, 2, fields, 2, *TILE), vm(slots, fields, NX, *TILE), vm(slots, 2, *TILE),
        vm(slots, 2, fields, *TILE), vm(slots, 2, 2, *TILE), vm(slots, 2, *TILE),
        dma((count,)), dma((slots, count)),
    ]


def body(source, sigma_intra, sigma_extra, membrane):
    sizes = tuple(lax.axis_size(a) for a in AXES)
    f32 = jnp.float32
    vm = lambda *s: pltpu.VMEM(s, f32)
    dma = pltpu.SemaphoreType.DMA
    out = jax.ShapeDtypeStruct(source.shape, f32)
    count = len(TILES)
    return pl.pallas_call(
        functools.partial(cycle_kernel, sizes),
        out_shape=(out, out),
        in_specs=[pl.BlockSpec(memory_space=pl.ANY)] * 4,
        out_specs=(pl.BlockSpec(memory_space=pltpu.VMEM),) * 2,
        scratch_shapes=[
            vm(KRYLOV + 1, 2, NX, *TILE), vm(2, count, 6, *TILE), vm(count, 4, *TILE), vm(NX, *TILE),
            *halo_scratch(FIELDS, 1), *halo_scratch(2, 2),
            vm(KRYLOV + 1, 16, NZ), vm(128, NZ), vm(3, *TILE), vm(3, 8, *TILE),
            dma((4,)), dma((3, 8)), dma((3, 8)),
        ],
        compiler_params=pltpu.CompilerParams(collective_id=0, has_side_effects=True),
    )(source, sigma_intra, sigma_extra, membrane)


def solution(mesh):
    return jax.shard_map(
        body,
        mesh=mesh,
        in_specs=(
            P(None, "gx", "gy", "gz"),
            P(None, "gx", "gy", "gz"),
            P(None, "gx", "gy", "gz"),
            P("gx", "gy", "gz"),
        ),
        out_specs=(P(None, "gx", "gy", "gz"), P(None, "gx", "gy", "gz")),
        check_vma=False,
    )
```

```python
import functools
import itertools

import jax
import jax.numpy as jnp
from jax import lax
from jax.experimental import pallas as pl
from jax.experimental.pallas import tpu as pltpu
from jax.sharding import PartitionSpec as P

KRYLOV = 10
AXES = ("gx", "gy", "gz")
MESH = pl.DeviceIdType.MESH
NX, NY, NZ = 4, 8, 128
TILE = (NY, NZ)
OWN, BESIDE = 0, 1
DIRECTIONS = [
    d for d in itertools.product((-1, 0, 1), repeat=3) if 1 <= sum(abs(a) for a in d) <= 2
]
TILES = (
    [(x, OWN, OWN) for x in range(-1, NX + 1)]
    + [(x, BESIDE, OWN) for x in range(NX)]
    + [(x, OWN, BESIDE) for x in range(NX)]
)
PLACE = {t: n for n, t in enumerate(TILES)}
FIELDS = 7
FACES = [d for d in DIRECTIONS if sum(abs(a) for a in d) == 1]
EDGES = [d for d in DIRECTIONS if sum(abs(a) for a in d) == 2]


class Halo:
    def __init__(self, refs, where, sizes):
        (self.own, self.pack, self.gx, self.gy, self.gz, self.gxy, self.gxz, self.gyz,
         self.send_sem, self.recv_sem) = refs
        self.where, self.sizes, self.count = where, sizes, 0

    def exists(self, direction):
        there = None
        for axis, step in enumerate(direction):
            if step:
                at = self.where[axis]
                ok = at > 0 if step < 0 else at < self.sizes[axis] - 1
                there = ok if there is None else jnp.logical_and(there, ok)
        return there

    def add(self, direction, ends):
        n = self.count
        self.count += 1

        def copy(slot):
            src, dst = ends(slot)
            return pltpu.make_async_remote_copy(
                src_ref=src, dst_ref=dst,
                send_sem=self.send_sem.at[n], recv_sem=self.recv_sem.at[slot, n],
                device_id={AXES[a]: self.where[a] + d for a, d in enumerate(direction) if d},
                device_id_type=MESH,
            )

        return direction, copy

    def planes(self, d, fields, first, count):
        low = NX - first - count if d[0] > 0 else first
        at = 2 - first - count if d[0] > 0 else first
        ghost = 0 if d[0] > 0 else 1
        return self.add(d, lambda slot: (
            self.own.at[fields, pl.ds(low, count)],
            self.gx.at[slot, ghost, fields, pl.ds(at, count)],
        ))

    def rows(self, d, fields, first, count):
        rows = pl.ds(NY - first - count if d[1] > 0 else first, count)
        return self.add(d, lambda slot: (
            self.own.at[fields, :, rows, :], self.gy.at[slot, fields, :, rows, :]
        ))

    def columns(self, d):
        return self.add(d, lambda slot: (self.pack, self.gz.at[slot, 0 if d[2] > 0 else 1]))

    def edge(self, d):
        dx, dy, dz = d
        ghost_x, ghost_z = (0 if dx > 0 else 1), (0 if dz > 0 else 1)
        row = pl.ds(NY - 1 if dy > 0 else 0, 1)
        if dx and dy:
            plane = NX - 1 if dx > 0 else 0
            return self.add(d, lambda slot: (
                self.own.at[:, plane, row, :], self.gxy.at[slot, ghost_x, :, row, :]
            ))
        if dx:
            return self.add(d, lambda slot: (self.pack, self.gxz.at[slot, ghost_x, ghost_z]))
        return self.add(d, lambda slot: (self.pack.at[row, :], self.gyz.at[slot, ghost_z, row, :]))

    def fill_pack(self, values):
        group = lax.broadcasted_iota(jnp.int32, TILE, 1) // 4
        packed = None
        for q, v in enumerate(values):
            moved = pltpu.roll(v, 4 * q + 2, 1)
            packed = moved if packed is None else jnp.where(group == q, moved, packed)
        self.pack[...] = packed

    def start(self, slot, messages):
        for d, copy in messages:
            @pl.when(self.exists(d))
            def _(copy=copy):
                copy(slot).start()

    def sent(self, slot, messages):
        for d, copy in messages:
            @pl.when(self.exists(d))
            def _(copy=copy):
                copy(slot).wait_send()

    def arrived(self, slot, messages):
        for d, copy in messages:
            @pl.when(self.exists(tuple(-a for a in d)))
            def _(copy=copy):
                copy(slot).wait_recv()

    def view(self, slot):
        return View(self, slot)


class View:
    def __init__(self, halo, slot):
        pair = lax.broadcasted_iota(jnp.int32, TILE, 1) % 4 < 2
        self.halo, self.slot, self.made = halo, slot, {}
        self.merge = lambda ref, *at: jnp.where(pair, ref[(slot, *at, 0)], ref[(slot, *at, 1)])
        self.merged = {}

    def columns(self, name, *at):
        if (name, at) not in self.merged:
            self.merged[name, at] = self.merge(getattr(self.halo, name), *at)
        return self.merged[name, at]

    def tile(self, f, x, ty, tz, turn=0):
        key = (f, x, ty, tz, turn)
        if key not in self.made:
            self.made[key] = self.make(f, x, ty, tz, turn)
        return self.made[key]

    def make(self, f, x, ty, tz, turn):
        h = self.halo
        if tz == BESIDE:
            if ty == BESIDE:
                source, plane = self.columns("gyz"), x
            elif x < 0:
                source, plane = self.columns("gxz", 0), NX - 1
            elif x >= NX:
                source, plane = self.columns("gxz", 1), 0
            else:
                source, plane = self.columns("gz"), x
            return pltpu.roll(source, (NZ - (4 * (f * NX + plane) + 2) + turn) % NZ, 1)
        if turn:
            return pltpu.roll(self.tile(f, x, ty, tz), turn % NZ, 1)
        if ty == BESIDE:
            if x < 0:
                return h.gxy[self.slot, 0, f]
            if x >= NX:
                return h.gxy[self.slot, 1, f]
            return h.gy[self.slot, f, x]
        if x < 0:
            return h.gx[self.slot, 0, f, x + 2]
        if x >= NX:
            return h.gx[self.slot, 1, f, x - NX]
        return h.own[f, x]


class Values:
    def __init__(self, values):
        self.values, self.made = values, {}

    def tile(self, f, x, ty, tz, turn=0):
        v = self.values[f][x, ty, tz]
        if not turn:
            return v
        key = (f, x, ty, tz, turn)
        if key not in self.made:
            self.made[key] = pltpu.roll(v, turn % NZ, 1)
        return self.made[key]


def beside(view, f, t, axis, step):
    x, ty, tz = t
    if axis == 0:
        return view.tile(f, x + step, ty, tz)
    if axis == 1:
        edge = lax.broadcasted_iota(jnp.int32, TILE, 0) == (0 if step < 0 else NY - 1)
        shift = 1 if step < 0 else NY - 1
        return jnp.where(
            edge,
            pltpu.roll(view.tile(f, x, 1 - ty, tz), shift, 0),
            pltpu.roll(view.tile(f, x, ty, tz), shift, 0),
        )
    edge = lax.broadcasted_iota(jnp.int32, TILE, 1) == (0 if step < 0 else NZ - 1)
    return jnp.where(edge, view.tile(f, x, ty, 1 - tz, -step), view.tile(f, x, ty, tz, -step))


def two_sum(a, b):
    s = a + b
    t = s - a
    return s, (a - (s - t)) + (b - t)


def add_pair(a, b):
    s, e = two_sum(a[0], b[0])
    return s, e + (a[1] + b[1])


def halves(a):
    c = 4097.0 * a
    top = c - (c - a)
    return top, a - top


def product(a, b, a_halves, b_halves):
    (ah, al), (bh, bl) = a_halves, b_halves
    p = a * b
    return p, ((ah * bh - p) + ah * bl + al * bh) + al * bl


class Pair:
    def __init__(self, high, low):
        self.high, self.low = two_sum(high, low)
        self.halves = halves(self.high)

    def times(self, other):
        p, e = product(self.high, other.high, self.halves, other.halves)
        return p, e + (self.high * other.low + self.low * other.high)


def minimizer(high, low):
    size = KRYLOV + 1
    row = lax.broadcasted_iota(jnp.int32, TILE, 0)
    col = lax.broadcasted_iota(jnp.int32, TILE, 1)
    groups = (NY + 3 - 1, 2)
    assert groups[0] == size - 1

    def column(j, group):
        i = groups[group] - row
        mask = col == lax.shift_right_arithmetic(i * (i + 1), 1) + j
        return tuple(
            jnp.broadcast_to(jnp.sum(jnp.where(mask, v, 0.0), axis=1, keepdims=True), TILE)
            for v in (high, low)
        )

    def place(i):
        return (0, groups[0] - i) if i > groups[1] else (1, groups[1] - i)

    def entry(vectors, i):
        group, r = place(i)
        return tuple(jnp.broadcast_to(v[r : r + 1, :], TILE) for v in vectors[group])

    columns = [{g: column(j, g) for g in range(2) if g == 0 or j <= groups[1]} for j in range(size)]
    first = entry(columns[0], 0)
    right = {0: first, 1: first}
    factors, solved = [], []
    for k in range(size):
        pivot = Pair(*entry(columns[k], k))
        guess = 1.0 / pivot.high
        p, e = product(pivot.high, guess, pivot.halves, halves(guess))
        inverse = Pair(guess, guess * (((1.0 - p) - e) - pivot.low * guess))
        bk = Pair(*entry(right, k))
        solved.append(sum(bk.times(inverse)))
        live = [g for g in range(2) if (g == 0 and k < size - 1) or (g == 1 and k < groups[1])]
        factor = {g: Pair(*Pair(*columns[k][g]).times(inverse)) for g in live}
        factors.append({g: (factor[g].high, factor[g].low) for g in live})
        targets = [(columns[j], Pair(*entry(columns[k], j))) for j in range(k + 1, size)]
        for target, by in targets + [(right, bk)]:
            for g in live:
                if g in target:
                    p, e = factor[g].times(by)
                    s, t = two_sum(target[g][0], -p)
                    target[g] = s, target[g][1] + (t - e)
    z = [None] * size
    for k in range(size - 1, -1, -1):
        rest = solved[k]
        for i in range(size - 1, k, -1):
            rest = rest - entry(factors[k], i)[0] * z[i]
        z[k] = rest
    return z


def cycle_kernel(
    sizes,
    source_hbm, intra_hbm, extra_hbm, membrane_hbm,
    solution_ref, residual_ref, scale_ref,
    basis, coef, block, inverse,
    s_own, s_pack, s_gx, s_gy, s_gz, s_gxy, s_gxz, s_gyz, s_send, s_recv,
    u_own, u_pack, u_gx, u_gy, u_gz, u_gxy, u_gxz, u_gyz, u_send, u_recv,
    gram_rows, gram_all, mine, parts,
    local_sem, sum_send, sum_recv,
):
    where = [lax.axis_index(a) for a in AXES]
    cells = Halo(
        (s_own, s_pack, s_gx, s_gy, s_gz, s_gxy, s_gxz, s_gyz, s_send, s_recv), where, sizes
    )
    halo = Halo(
        (u_own, u_pack, u_gx, u_gy, u_gz, u_gxy, u_gxz, u_gyz, u_send, u_recv), where, sizes
    )

    every = slice(None)
    near, rest, messages = [], [], []
    for d in FACES:
        if d[0]:
            near.append(cells.planes(d, pl.ds(0, 2), 0, 1))
            rest.append(cells.planes(d, pl.ds(2, 5), 0, 1))
            rest.append(cells.planes(d, pl.ds(0, 2), 1, 1))
        elif d[1]:
            near.append(cells.rows(d, pl.ds(2, 2), 0, 1))
            rest.append(cells.rows(d, pl.ds(0, 2), 0, 1))
            rest.append(cells.rows(d, pl.ds(4, 3), 0, 1))
            rest.append(cells.rows(d, pl.ds(2, 2), 1, 1))
        else:
            near.append(cells.columns(d))
    for d in EDGES:
        rest.append(cells.edge(d))
        messages.append(halo.edge(d))
    for d in FACES:
        if d[0]:
            messages.append(halo.planes(d, every, 0, 2))
        elif d[1]:
            messages.append(halo.rows(d, every, 0, 2))
        else:
            messages.append(halo.columns(d))

    loads = [
        pltpu.make_async_copy(ref.at[axis], s_own.at[2 * axis + s], local_sem.at[2 * axis + s])
        for axis in range(3) for s, ref in enumerate((intra_hbm, extra_hbm))
    ] + [
        pltpu.make_async_copy(membrane_hbm, s_own.at[6], local_sem.at[6]),
        pltpu.make_async_copy(source_hbm, basis.at[0], local_sem.at[7]),
    ]
    for c in loads:
        c.start()
    for h in (cells, halo):
        for ref in (h.gx, h.gy, h.gz, h.gxy, h.gxz, h.gyz):
            ref[...] = jnp.zeros_like(ref)

    barrier = pltpu.get_barrier_semaphore()
    expected = 0
    for d in DIRECTIONS:
        there = cells.exists(d)
        expected = expected + jnp.where(there, 1, 0)

        @pl.when(there)
        def _(d=d):
            pl.semaphore_signal(
                barrier, inc=1,
                device_id={AXES[a]: where[a] + step for a, step in enumerate(d) if step},
                device_id_type=MESH,
            )
    gram_all[...] = jnp.zeros_like(gram_all)
    for k in range(1, KRYLOV + 1):
        basis[k] = jnp.zeros_like(basis.at[k])
    for c in loads:
        c.wait()
    cells.fill_pack([s_own[f, x] for f in range(FIELDS) for x in range(NX)])
    pl.semaphore_wait(barrier, expected)

    cells.start(0, near)
    cells.start(0, rest)

    def coefficients(view, beside, tiles):
        for t in tiles:
            n = PLACE[t]
            diagonals = []
            for s in range(2):
                total = None
                for axis in range(3):
                    here = view.tile(2 * axis + s, *t)
                    lower = 0.5 * (here + beside(view, 2 * axis + s, t, axis, -1))
                    upper = 0.5 * (here + beside(view, 2 * axis + s, t, axis, 1))
                    coef[s, n, 2 * axis] = lower
                    coef[s, n, 2 * axis + 1] = upper
                    total = upper + lower if total is None else total + upper + lower
                diagonals.append(total)
            di, de, m = diagonals[0], diagonals[1], view.tile(6, *t)
            det = m * di + m * de + di * de
            inside = m > 0.0
            over = jnp.where(inside, 1.0 / jnp.where(inside, det, 1.0), 0.0)
            block[n, 0] = de * over
            block[n, 1] = m * over
            block[n, 2] = -di * over
            block[n, 3] = (m + di) * over
            if t in own:
                inverse[t[0]] = (di + de) * over

    def beside_own(view, f, t, axis, step):
        if axis != 1:
            return beside(view, f, t, axis, step)
        row = NY - 1 if step < 0 else 0
        edge = lax.broadcasted_iota(jnp.int32, TILE, 0) == NY - 1 - row
        ghost = s_gy[0, f, t[0], pl.ds(row, 1), :]
        return jnp.where(edge, ghost, pltpu.roll(view.tile(f, *t), 1 if step < 0 else NY - 1, 0))

    own = [(x, OWN, OWN) for x in range(NX)]
    def solved(t, a, b):
        n = PLACE[t]
        return block[n, 0] * a + block[n, 1] * b, block[n, 2] * a + block[n, 3] * b

    def apply(view, t):
        n = PLACE[t]
        off = []
        for s in range(2):
            total = None
            for axis in range(3):
                for side, step in enumerate((-1, 1)):
                    term = coef[s, n, 2 * axis + side] * beside(view, s, t, axis, step)
                    total = term if total is None else total + term
            off.append(total)
        return off[0], off[0] + off[1]

    def load(k):
        return [[basis[k, s, x] for x in range(NX)] for s in range(2)]

    def keep(k, v):
        for s in range(2):
            for x in range(NX):
                basis[k, s, x] = v[s][x]

    def stage(v):
        values = [[None] * NX for _ in range(2)]
        for x in range(NX):
            values[0][x], values[1][x] = solved(own[x], v[0][x], v[1][x])
        for s in range(2):
            for x in range(NX):
                u_own[s, x] = values[s][x]
        halo.fill_pack(values[0] + values[1])

    def gram_row(k):
        at = load(k)
        for i in range(KRYLOV + 1):
            total = None
            for s in range(2):
                for x in range(NX):
                    term = at[s][x] * basis[i, s, x]
                    total = term if total is None else total + term
            gram_rows[k, pl.ds(i, 1), :] = jnp.sum(total, axis=0, keepdims=True)

    def two_steps(slot):
        view = halo.view(slot)
        first, next_u = {}, [{}, {}]
        for t in TILES:
            first[t] = apply(view, t)
            next_u[0][t], next_u[1][t] = solved(t, *first[t])
        values = Values(next_u)
        second = [apply(values, t) for t in own]
        return (
            [[first[t][s] for t in own] for s in range(2)],
            [[second[x][s] for x in range(NX)] for s in range(2)],
        )

    def combine(f, *vs):
        return [[f(*(v[s][x] for v in vs)) for x in range(NX)] for s in range(2)]

    def advance(k, slot):
        w, b = two_steps(slot)
        odd = combine(lambda p, q: 2.0 * p - q, w, load(k - 1))
        even = combine(lambda p, q, r: 4.0 * p - 2.0 * q - r, b, load(k), load(k - 2))
        return odd, even

    cells.arrived(0, near)
    coefficients(cells.view(0), beside_own, own)
    stage(load(0))
    halo.start(0, messages)
    gram_row(0)
    cells.sent(0, near + rest)
    cells.arrived(0, rest)
    coefficients(cells.view(0), beside, [t for t in TILES if t not in own])
    halo.sent(0, messages)
    halo.arrived(0, messages)
    odd, b = two_steps(0)
    even = combine(lambda p, q: 2.0 * p - q, b, load(0))
    stage(even)
    halo.start(1, messages)
    keep(1, odd)
    keep(2, even)

    def step(r, carry):
        k, slot = 2 * r, lax.rem(r, 2)
        gram_row(k - 1)
        gram_row(k)
        halo.sent(slot, messages)
        halo.arrived(slot, messages)
        odd, even = advance(k, slot)
        stage(even)
        halo.start(1 - slot, messages)
        keep(k + 1, odd)
        keep(k + 2, even)
        return carry

    rounds = KRYLOV // 2
    lax.fori_loop(1, rounds - 1, step, 0)
    gram_row(KRYLOV - 3)
    gram_row(KRYLOV - 2)
    last = (rounds - 1) % 2
    halo.sent(last, messages)
    halo.arrived(last, messages)
    odd, even = advance(KRYLOV - 2, last)
    keep(KRYLOV - 1, odd)
    keep(KRYLOV, even)
    gram_row(KRYLOV - 1)
    gram_row(KRYLOV)

    at = 0
    for k in range(KRYLOV + 1):
        gram_all[pl.ds(at, k + 1), :] = gram_rows[k, pl.ds(0, k + 1), :]
        at += k + 1
    ones = jnp.ones(TILE, jnp.bfloat16)
    left, totals = gram_all[...], []
    for _ in range(3):
        piece = left.astype(jnp.bfloat16)
        left = left - piece.astype(jnp.float32)
        totals.append(lax.dot_general(
            ones, piece, (((1,), (1,)), ((), ())), preferred_element_type=jnp.float32
        )[0:1, :])
    high, low = two_sum(totals[0], totals[1])
    low = low + totals[2]
    for n, d in enumerate((2, 1, 0)):
        size = sizes[d]
        mine[n, 0:1, :] = high
        mine[n, 1:2, :] = low
        parts[n, where[d], 0:1, :] = high
        parts[n, where[d], 1:2, :] = low

        def copy(j, slot, other):
            return pltpu.make_async_remote_copy(
                src_ref=mine.at[n, pl.ds(0, 2), :], dst_ref=parts.at[n, slot, pl.ds(0, 2), :],
                send_sem=sum_send.at[n, j], recv_sem=sum_recv.at[n, slot],
                device_id={AXES[d]: other}, device_id_type=MESH,
            )

        others = [(j, lax.rem(where[d] + j, size)) for j in range(1, size)]
        for j, other in others:
            copy(j, where[d], other).start()
        for j, other in others:
            copy(j, other, other).wait_recv()
        for j, other in others:
            copy(j, where[d], other).wait_send()
        terms = [(parts[n, j, 0:1, :], parts[n, j, 1:2, :]) for j in range(size)]
        while len(terms) > 1:
            terms = [add_pair(terms[i], terms[i + 1]) for i in range(0, len(terms), 2)]
        high, low = two_sum(*terms[0])

    z = minimizer(jnp.broadcast_to(high, TILE), jnp.broadcast_to(low, TILE))
    size = KRYLOV + 1
    total = z[0]
    for k in range(1, size):
        total = total + z[k]
    scale_ref[...] = 1.0 / total
    rho = z
    slope = [None] * size
    running = jnp.zeros(TILE, jnp.float32)
    weighted = jnp.zeros(TILE, jnp.float32)
    for j in range(KRYLOV - 1, -1, -1):
        running = running + rho[j + 1]
        weighted = weighted + running
        slope[j] = weighted
    coeffs = [slope[0]] + [2.0 * slope[j] for j in range(1, KRYLOV)]

    for x in range(NX):
        combined = []
        for s in range(2):
            vectors = [basis[k, s, x] for k in range(size)]
            r = rho[0] * vectors[0]
            c = coeffs[0] * vectors[0]
            for k in range(1, size):
                r = r + rho[k] * vectors[k]
                if k < KRYLOV:
                    c = c + coeffs[k] * vectors[k]
            residual_ref[s, x] = r
            combined.append(c)
        n = PLACE[own[x]]
        solution_ref[0, x] = inverse[x] * combined[0] + block[n, 2] * combined[1]
        solution_ref[1, x] = block[n, 2] * combined[0] + block[n, 3] * combined[1]


def halo_scratch(fields, slots, count):
    vm = lambda *s: pltpu.VMEM(s, jnp.float32)
    dma = pltpu.SemaphoreType.DMA
    return [
        vm(fields, NX, *TILE), vm(*TILE),
        vm(slots, 2, fields, 2, *TILE), vm(slots, fields, NX, *TILE), vm(slots, 2, *TILE),
        vm(slots, 2, fields, *TILE), vm(slots, 2, 2, *TILE), vm(slots, 2, *TILE),
        dma((count,)), dma((slots, count)),
    ]


def body(source, sigma_intra, sigma_extra, membrane):
    sizes = tuple(lax.axis_size(a) for a in AXES)
    f32 = jnp.float32
    vm = lambda *s: pltpu.VMEM(s, f32)
    dma = pltpu.SemaphoreType.DMA
    count = len(TILES)
    unscaled, remainder, scale = pl.pallas_call(
        functools.partial(cycle_kernel, sizes),
        out_shape=(vm(*source.shape), vm(*source.shape), vm(*TILE)),
        in_specs=[pl.BlockSpec(memory_space=pl.ANY)] * 4,
        out_specs=(pl.BlockSpec(memory_space=pltpu.VMEM),) * 3,
        scratch_shapes=[
            vm(KRYLOV + 1, 2, NX, *TILE), vm(2, count, 6, *TILE), vm(count, 4, *TILE), vm(NX, *TILE),
            *halo_scratch(FIELDS, 1, 28), *halo_scratch(2, 2, len(DIRECTIONS)),
            vm(KRYLOV + 1, 16, NZ), vm(128, NZ), vm(3, *TILE), vm(3, 8, *TILE),
            dma((8,)), dma((3, 8)), dma((3, 8)),
        ],
        compiler_params=pltpu.CompilerParams(collective_id=0, has_side_effects=True),
    )(source, sigma_intra, sigma_extra, membrane)
    return unscaled * scale, remainder * scale


def solution(mesh):
    return jax.shard_map(
        body,
        mesh=mesh,
        in_specs=(
            P(None, "gx", "gy", "gz"),
            P(None, "gx", "gy", "gz"),
            P(None, "gx", "gy", "gz"),
            P("gx", "gy", "gz"),
        ),
        out_specs=(P(None, "gx", "gy", "gz"), P(None, "gx", "gy", "gz")),
        check_vma=False,
    )
```

```python
import functools
import itertools

import jax
import jax.numpy as jnp
from jax import lax
from jax.experimental import pallas as pl
from jax.experimental.pallas import tpu as pltpu
from jax.sharding import PartitionSpec as P

KRYLOV = 10
AXES = ("gx", "gy", "gz")
MESH = pl.DeviceIdType.MESH
NX, NY, NZ = 4, 8, 128
TILE = (NY, NZ)
OWN, BESIDE = 0, 1
FACES, EDGES, CORNERS = (
    [d for d in itertools.product((-1, 0, 1), repeat=3) if sum(abs(a) for a in d) == n]
    for n in (1, 2, 3)
)
DIRECTIONS = FACES + EDGES + CORNERS
FIELDS = 7
SHALLOW, DEEP = 2, 4


def tiles(reach):
    return [
        (x, ty, tz)
        for ty in (OWN, BESIDE) for tz in (OWN, BESIDE) for x in range(-reach, NX + reach)
        if max(-x, x - NX + 1, 0) + ty + tz <= reach
    ]


TILES = tiles(DEEP - 1)
PLACE = {t: n for n, t in enumerate(TILES)}


def toward(where, sizes, direction):
    return {
        AXES[a]: lax.rem(where[a] + step + sizes[a], sizes[a])
        for a, step in enumerate(direction) if step
    }


class Halo:
    def __init__(self, depth, refs, where, sizes):
        (self.own, self.pack, self.gx, self.gy, self.gz, self.gxy, self.gxz, self.gyz, self.gxyz,
         self.send_sem, self.recv_sem) = refs
        self.depth, self.stride, self.each = depth, 2 * depth, NZ // (2 * depth)
        self.where, self.sizes, self.count = where, sizes, 0

    def exists(self, direction):
        there = None
        for axis, step in enumerate(direction):
            if step:
                at = self.where[axis]
                ok = at > 0 if step < 0 else at < self.sizes[axis] - 1
                there = ok if there is None else jnp.logical_and(there, ok)
        return there

    def add(self, direction, ends):
        n = self.count
        self.count += 1

        def copy(slot):
            src, dst = ends(slot)
            return pltpu.make_async_remote_copy(
                src_ref=src, dst_ref=dst,
                send_sem=self.send_sem.at[n], recv_sem=self.recv_sem.at[slot, n],
                device_id=toward(self.where, self.sizes, direction),
                device_id_type=MESH,
            )

        return direction, copy

    def planes(self, d, fields, first, count):
        low = NX - first - count if d[0] > 0 else first
        at = self.depth - first - count if d[0] > 0 else first
        ghost = 0 if d[0] > 0 else 1
        return self.add(d, lambda slot: (
            self.own.at[fields, pl.ds(low, count)],
            self.gx.at[slot, ghost, fields, pl.ds(at, count)],
        ))

    def rows(self, d, fields, first, count):
        rows = pl.ds(NY - first - count if d[1] > 0 else first, count)
        return self.add(d, lambda slot: (
            self.own.at[fields, :, rows, :], self.gy.at[slot, fields, :, rows, :]
        ))

    def columns(self, d):
        return self.add(d, lambda slot: (self.pack, self.gz.at[slot, 0 if d[2] > 0 else 1]))

    def edge(self, d):
        dx, dy, dz = d
        ghost_x, ghost_z = (0 if dx > 0 else 1), (0 if dz > 0 else 1)
        count = self.depth - sum(abs(a) for a in d) + 1
        row = pl.ds(NY - count if dy > 0 else 0, count)
        if not dz:
            planes = pl.ds(NX - count if dx > 0 else 0, count)
            return self.add(d, lambda slot: (
                self.own.at[:, planes, row, :], self.gxy.at[slot, ghost_x, :, :, row, :]
            ))
        if not dy:
            return self.add(d, lambda slot: (self.pack, self.gxz.at[slot, ghost_x, ghost_z]))
        if not dx:
            return self.add(d, lambda slot: (
                self.pack.at[:, row, :], self.gyz.at[slot, ghost_z, :, row, :]
            ))
        return self.add(d, lambda slot: (
            self.pack.at[:, row, :], self.gxyz.at[slot, ghost_x, ghost_z, :, row, :]
        ))

    def fill_pack(self, values):
        group = lax.broadcasted_iota(jnp.int32, TILE, 1) // self.stride
        for first in range(0, len(values), self.each):
            packed = None
            for q, v in enumerate(values[first : first + self.each]):
                moved = pltpu.roll(v, self.stride * q + self.depth, 1)
                packed = moved if packed is None else jnp.where(group == q, moved, packed)
            self.pack[first // self.each] = packed

    def start(self, slot, messages):
        for d, copy in messages:
            @pl.when(self.exists(d))
            def _(copy=copy):
                copy(slot).start()

    def sent(self, slot, messages):
        for d, copy in messages:
            @pl.when(self.exists(d))
            def _(copy=copy):
                copy(slot).wait_send()

    def arrived(self, slot, messages):
        for d, copy in messages:
            @pl.when(self.exists(tuple(-a for a in d)))
            def _(copy=copy):
                copy(slot).wait_recv()

    def view(self, slot):
        return View(self, slot)


class View:
    def __init__(self, halo, slot):
        self.halo, self.slot, self.made, self.merged = halo, slot, {}, {}

    def columns(self, name, *at):
        if (name, at) not in self.merged:
            h, (*before, pack) = self.halo, at
            ref = getattr(h, name)
            low = lax.broadcasted_iota(jnp.int32, TILE, 1) % h.stride < h.depth
            self.merged[name, at] = jnp.where(
                low, ref[(self.slot, *before, 0, pack)], ref[(self.slot, *before, 1, pack)]
            )
        return self.merged[name, at]

    def tile(self, f, x, ty, tz, turn=0):
        key = (f, x, ty, tz, turn)
        if key not in self.made:
            self.made[key] = self.make(f, x, ty, tz, turn)
        return self.made[key]

    def make(self, f, x, ty, tz, turn):
        h = self.halo
        outside = (0,) if x < 0 else (1,) if x >= NX else ()
        if tz == BESIDE:
            pack, q = divmod(f * NX + x % NX, h.each)
            name = "g" + ("x" if outside else "") + ("y" if ty == BESIDE else "") + "z"
            source = self.columns(name, *outside, pack)
            return pltpu.roll(source, (turn - h.stride * q - h.depth) % NZ, 1)
        if turn:
            return pltpu.roll(self.tile(f, x, ty, tz), turn % NZ, 1)
        if ty == BESIDE:
            if not outside:
                return h.gy[self.slot, f, x]
            return h.gxy[self.slot, outside[0], f, x + h.depth - 1 if x < 0 else x - NX]
        if not outside:
            return h.own[f, x]
        return h.gx[self.slot, outside[0], f, x + h.depth if x < 0 else x - NX]


class Values:
    def __init__(self, values):
        self.values, self.made = values, {}

    def tile(self, f, x, ty, tz, turn=0):
        v = self.values[f][x, ty, tz]
        if not turn:
            return v
        key = (f, x, ty, tz, turn)
        if key not in self.made:
            self.made[key] = pltpu.roll(v, turn % NZ, 1)
        return self.made[key]


def beside(view, f, t, axis, step):
    x, ty, tz = t
    if axis == 0:
        return view.tile(f, x + step, ty, tz)
    if axis == 1:
        edge = lax.broadcasted_iota(jnp.int32, TILE, 0) == (0 if step < 0 else NY - 1)
        shift = 1 if step < 0 else NY - 1
        return jnp.where(
            edge,
            pltpu.roll(view.tile(f, x, 1 - ty, tz), shift, 0),
            pltpu.roll(view.tile(f, x, ty, tz), shift, 0),
        )
    edge = lax.broadcasted_iota(jnp.int32, TILE, 1) == (0 if step < 0 else NZ - 1)
    return jnp.where(edge, view.tile(f, x, ty, 1 - tz, -step), view.tile(f, x, ty, tz, -step))


def two_sum(a, b):
    s = a + b
    t = s - a
    return s, (a - (s - t)) + (b - t)


def add_pair(a, b):
    s, e = two_sum(a[0], b[0])
    return s, e + (a[1] + b[1])


def halves(a):
    c = 4097.0 * a
    top = c - (c - a)
    return top, a - top


def product(a, b, a_halves, b_halves):
    (ah, al), (bh, bl) = a_halves, b_halves
    p = a * b
    return p, ((ah * bh - p) + ah * bl + al * bh) + al * bl


class Pair:
    def __init__(self, high, low):
        self.high, self.low = two_sum(high, low)
        self.halves = halves(self.high)

    def times(self, other):
        p, e = product(self.high, other.high, self.halves, other.halves)
        return p, e + (self.high * other.low + self.low * other.high)


def minimizer(high, low):
    size = KRYLOV + 1
    row = lax.broadcasted_iota(jnp.int32, TILE, 0)
    col = lax.broadcasted_iota(jnp.int32, TILE, 1)
    groups = (NY + 3 - 1, 2)
    assert groups[0] == size - 1

    def column(j, group):
        i = groups[group] - row
        mask = col == lax.shift_right_arithmetic(i * (i + 1), 1) + j
        return tuple(
            jnp.broadcast_to(jnp.sum(jnp.where(mask, v, 0.0), axis=1, keepdims=True), TILE)
            for v in (high, low)
        )

    def place(i):
        return (0, groups[0] - i) if i > groups[1] else (1, groups[1] - i)

    def entry(vectors, i):
        group, r = place(i)
        return tuple(jnp.broadcast_to(v[r : r + 1, :], TILE) for v in vectors[group])

    columns = [{g: column(j, g) for g in range(2) if g == 0 or j <= groups[1]} for j in range(size)]
    first = entry(columns[0], 0)
    right = {0: first, 1: first}
    factors, solved = [], []
    for k in range(size):
        pivot = Pair(*entry(columns[k], k))
        guess = 1.0 / pivot.high
        p, e = product(pivot.high, guess, pivot.halves, halves(guess))
        inverse = Pair(guess, guess * (((1.0 - p) - e) - pivot.low * guess))
        bk = Pair(*entry(right, k))
        solved.append(sum(bk.times(inverse)))
        live = [g for g in range(2) if (g == 0 and k < size - 1) or (g == 1 and k < groups[1])]
        factor = {g: Pair(*Pair(*columns[k][g]).times(inverse)) for g in live}
        factors.append({g: (factor[g].high, factor[g].low) for g in live})
        targets = [(columns[j], Pair(*entry(columns[k], j))) for j in range(k + 1, size)]
        for target, by in targets + [(right, bk)]:
            for g in live:
                if g in target:
                    p, e = factor[g].times(by)
                    s, t = two_sum(target[g][0], -p)
                    target[g] = s, target[g][1] + (t - e)
    z = [None] * size
    for k in range(size - 1, -1, -1):
        rest = solved[k]
        for i in range(size - 1, k, -1):
            rest = rest - entry(factors[k], i)[0] * z[i]
        z[k] = rest
    return z


def cycle_kernel(
    sizes,
    source_hbm, intra_hbm, extra_hbm, membrane_hbm,
    solution_ref, residual_ref, scale_ref,
    basis, coef, block, inverse,
    s_own, u_own, *refs,
):
    groups = [refs[10 * n : 10 * n + 10] for n in range(4)]
    gram_rows, gram_all, mine, parts, local_sem, sum_send, sum_recv = refs[40:]
    where = [lax.axis_index(a) for a in AXES]
    cells, deep_cells, halo, deep_halo = (
        Halo(depth, (own, *group), where, sizes)
        for depth, own, group in zip((SHALLOW, DEEP) * 2, (s_own, s_own, u_own, u_own), groups)
    )

    every = slice(None)
    near, rest, messages = [], [], []
    for d in FACES:
        if d[0]:
            near.append(cells.planes(d, pl.ds(0, 2), 0, 1))
            rest.append(cells.planes(d, pl.ds(2, 5), 0, 1))
            rest.append(cells.planes(d, pl.ds(0, 2), 1, 1))
        elif d[1]:
            near.append(cells.rows(d, pl.ds(2, 2), 0, 1))
            rest.append(cells.rows(d, pl.ds(0, 2), 0, 1))
            rest.append(cells.rows(d, pl.ds(4, 3), 0, 1))
            rest.append(cells.rows(d, pl.ds(2, 2), 1, 1))
        else:
            near.append(cells.columns(d))
    for d in EDGES:
        rest.append(cells.edge(d))

    def all_messages(h, trim):
        made = [h.edge(d) for d in (CORNERS if h.depth > 2 else []) + EDGES]
        for d in FACES:
            if d[0] and trim:
                made.append(h.planes(d, pl.ds(0, 2), 0, h.depth))
                made.append(h.planes(d, pl.ds(2, 5), 0, h.depth - 1))
            elif d[0]:
                made.append(h.planes(d, every, 0, h.depth))
            elif d[1]:
                made.append(h.rows(d, every, 0, h.depth))
            else:
                made.append(h.columns(d))
        return made

    messages = all_messages(halo, False)
    deep_rest = all_messages(deep_cells, True)
    deep_messages = all_messages(deep_halo, False)

    loads = [
        pltpu.make_async_copy(ref.at[axis], s_own.at[2 * axis + s], local_sem.at[2 * axis + s])
        for axis in range(3) for s, ref in enumerate((intra_hbm, extra_hbm))
    ] + [
        pltpu.make_async_copy(membrane_hbm, s_own.at[6], local_sem.at[6]),
        pltpu.make_async_copy(source_hbm, basis.at[0], local_sem.at[7]),
    ]
    for c in loads:
        c.start()
    for h in (cells, deep_cells, halo, deep_halo):
        for ref in (h.gx, h.gy, h.gz, h.gxy, h.gxz, h.gyz, h.gxyz):
            ref[...] = jnp.zeros_like(ref)

    barrier = pltpu.get_barrier_semaphore()
    expected = 0
    for d in DIRECTIONS:
        there = cells.exists(d)
        expected = expected + jnp.where(there, 1, 0)

        @pl.when(there)
        def _(d=d):
            pl.semaphore_signal(
                barrier, inc=1,
                device_id=toward(where, sizes, d),
                device_id_type=MESH,
            )
    for d in range(3):
        for far in range(6, sizes[d]):
            for step in (-far, far):
                there = where[d] >= far if step < 0 else where[d] < sizes[d] - far
                expected = expected + jnp.where(there, 1, 0)

                @pl.when(there)
                def _(d=d, step=step):
                    pl.semaphore_signal(
                        barrier, inc=1, device_id={AXES[d]: lax.rem(where[d] + step + sizes[d], sizes[d])}, device_id_type=MESH
                    )
    gram_all[...] = jnp.zeros_like(gram_all)
    for k in range(1, KRYLOV + 1):
        basis[k] = jnp.zeros_like(basis.at[k])
    for c in loads:
        c.wait()
    cells.fill_pack([s_own[f, x] for f in range(FIELDS) for x in range(NX)])
    pl.semaphore_wait(barrier, expected)

    cells.start(0, near)
    cells.start(0, rest)

    def coefficients(view, beside, tiles):
        for t in tiles:
            n = PLACE[t]
            diagonals = []
            for s in range(2):
                total = None
                for axis in range(3):
                    here = view.tile(2 * axis + s, *t)
                    lower = 0.5 * (here + beside(view, 2 * axis + s, t, axis, -1))
                    upper = 0.5 * (here + beside(view, 2 * axis + s, t, axis, 1))
                    coef[s, n, 2 * axis] = lower
                    coef[s, n, 2 * axis + 1] = upper
                    total = upper + lower if total is None else total + upper + lower
                diagonals.append(total)
            di, de, m = diagonals[0], diagonals[1], view.tile(6, *t)
            det = m * di + m * de + di * de
            inside = m > 0.0
            over = jnp.where(inside, 1.0 / jnp.where(inside, det, 1.0), 0.0)
            block[n, 0] = de * over
            block[n, 1] = m * over
            block[n, 2] = -di * over
            block[n, 3] = (m + di) * over
            if t in own:
                inverse[t[0]] = (di + de) * over

    def beside_own(view, f, t, axis, step):
        if axis != 1:
            return beside(view, f, t, axis, step)
        row = NY - 1 if step < 0 else 0
        edge = lax.broadcasted_iota(jnp.int32, TILE, 0) == NY - 1 - row
        ghost = cells.gy[0, f, t[0], pl.ds(row, 1), :]
        return jnp.where(edge, ghost, pltpu.roll(view.tile(f, *t), 1 if step < 0 else NY - 1, 0))

    own = [(x, OWN, OWN) for x in range(NX)]
    def solved(t, a, b):
        n = PLACE[t]
        return block[n, 0] * a + block[n, 1] * b, block[n, 2] * a + block[n, 3] * b

    def apply(view, t):
        n = PLACE[t]
        off = []
        for s in range(2):
            total = None
            for axis in range(3):
                for side, step in enumerate((-1, 1)):
                    term = coef[s, n, 2 * axis + side] * beside(view, s, t, axis, step)
                    total = term if total is None else total + term
            off.append(total)
        return off[0], off[0] + off[1]

    def load(k):
        return [[basis[k, s, x] for x in range(NX)] for s in range(2)]

    def keep(k, v):
        for s in range(2):
            for x in range(NX):
                basis[k, s, x] = v[s][x]

    def stage(h, v):
        values = [[None] * NX for _ in range(2)]
        for x in range(NX):
            values[0][x], values[1][x] = solved(own[x], v[0][x], v[1][x])
        for s in range(2):
            for x in range(NX):
                u_own[s, x] = values[s][x]
        h.fill_pack(values[0] + values[1])

    def gram_row(k):
        at = load(k)
        for i in range(KRYLOV + 1):
            total = None
            for s in range(2):
                for x in range(NX):
                    term = at[s][x] * basis[i, s, x]
                    total = term if total is None else total + term
            gram_rows[k, pl.ds(i, 1), :] = jnp.sum(total, axis=0, keepdims=True)

    def powers(h, slot):
        view, made = h.view(slot), []
        for reach in range(h.depth - 1, -1, -1):
            now = {t: apply(view, t) for t in tiles(reach)}
            made.append([[now[t][s] for t in own] for s in range(2)])
            if reach:
                then = {t: solved(t, *now[t]) for t in now}
                view = Values([{t: then[t][s] for t in then} for s in range(2)])
        return made

    def combine(f, *vs):
        return [[f(*(v[s][x] for v in vs)) for x in range(NX)] for s in range(2)]

    def advance(k, h, slot):
        here = load(k)
        made = powers(h, slot)
        terms = [
            made[0],
            combine(lambda b, a: 2.0 * b - a, made[1], here),
        ]
        if h.depth > 2:
            terms.append(combine(lambda b, a: 4.0 * b - 3.0 * a, made[2], made[0]))
            terms.append(combine(lambda b, a, r: 8.0 * b - 8.0 * a + r, made[3], made[1], here))
        if k == 0:
            return terms
        return [combine(lambda t, p: 2.0 * t - p, t, load(abs(k - 1 - j))) for j, t in enumerate(terms)]

    cells.arrived(0, near)
    coefficients(cells.view(0), beside_own, own)
    stage(halo, load(0))
    halo.start(0, messages)
    deep_cells.fill_pack([s_own[f, x] for f in range(FIELDS) for x in range(NX)])
    deep_cells.start(0, deep_rest)
    gram_row(0)
    cells.sent(0, near + rest)
    cells.arrived(0, rest)
    coefficients(cells.view(0), beside, [t for t in tiles(SHALLOW - 1) if t not in own])
    halo.sent(0, messages)
    halo.arrived(0, messages)
    made = advance(0, halo, 0)
    stage(deep_halo, made[-1])
    deep_halo.start(0, deep_messages)
    keep(1, made[0])
    keep(2, made[1])
    gram_row(1)
    gram_row(2)
    deep_cells.sent(0, deep_rest)
    deep_cells.arrived(0, deep_rest)
    coefficients(deep_cells.view(0), beside, [
        t for t in TILES if t[1] == BESIDE or t[2] == BESIDE or t not in tiles(SHALLOW - 1)
    ])
    for slot, k in enumerate((2, 6)):
        deep_halo.sent(slot, deep_messages)
        deep_halo.arrived(slot, deep_messages)
        made = advance(k, deep_halo, slot)
        if slot == 0:
            stage(deep_halo, made[-1])
            deep_halo.start(1, deep_messages)
        for j, v in enumerate(made):
            keep(k + 1 + j, v)
        for j in range(len(made)):
            gram_row(k + 1 + j)

    at = 0
    for k in range(KRYLOV + 1):
        gram_all[pl.ds(at, k + 1), :] = gram_rows[k, pl.ds(0, k + 1), :]
        at += k + 1
    ones = jnp.ones(TILE, jnp.bfloat16)
    left, totals = gram_all[...], []
    for _ in range(3):
        piece = left.astype(jnp.bfloat16)
        left = left - piece.astype(jnp.float32)
        totals.append(lax.dot_general(
            ones, piece, (((1,), (1,)), ((), ())), preferred_element_type=jnp.float32
        )[0:1, :])
    high, low = two_sum(totals[0], totals[1])
    low = low + totals[2]
    for n, d in enumerate((2, 1, 0)):
        size = sizes[d]
        mine[n, 0:1, :] = high
        mine[n, 1:2, :] = low
        parts[n, where[d], 0:1, :] = high
        parts[n, where[d], 1:2, :] = low

        def copy(j, slot, other):
            return pltpu.make_async_remote_copy(
                src_ref=mine.at[n, pl.ds(0, 2), :], dst_ref=parts.at[n, slot, pl.ds(0, 2), :],
                send_sem=sum_send.at[n, j], recv_sem=sum_recv.at[n, slot],
                device_id={AXES[d]: other}, device_id_type=MESH,
            )

        others = [(j, lax.rem(where[d] + j, size)) for j in range(1, size)]
        for j, other in others:
            copy(j, where[d], other).start()
        for j, other in others:
            copy(j, other, other).wait_recv()
        for j, other in others:
            copy(j, where[d], other).wait_send()
        terms = [(parts[n, j, 0:1, :], parts[n, j, 1:2, :]) for j in range(size)]
        while len(terms) > 1:
            terms = [add_pair(terms[i], terms[i + 1]) for i in range(0, len(terms), 2)]
        high, low = two_sum(*terms[0])

    z = minimizer(jnp.broadcast_to(high, TILE), jnp.broadcast_to(low, TILE))
    size = KRYLOV + 1
    total = z[0]
    for k in range(1, size):
        total = total + z[k]
    scale_ref[...] = 1.0 / total
    rho = z
    slope = [None] * size
    running = jnp.zeros(TILE, jnp.float32)
    weighted = jnp.zeros(TILE, jnp.float32)
    for j in range(KRYLOV - 1, -1, -1):
        running = running + rho[j + 1]
        weighted = weighted + running
        slope[j] = weighted
    coeffs = [slope[0]] + [2.0 * slope[j] for j in range(1, KRYLOV)]

    for x in range(NX):
        combined = []
        for s in range(2):
            vectors = [basis[k, s, x] for k in range(size)]
            r = rho[0] * vectors[0]
            c = coeffs[0] * vectors[0]
            for k in range(1, size):
                r = r + rho[k] * vectors[k]
                if k < KRYLOV:
                    c = c + coeffs[k] * vectors[k]
            residual_ref[s, x] = r
            combined.append(c)
        n = PLACE[own[x]]
        solution_ref[0, x] = inverse[x] * combined[0] + block[n, 2] * combined[1]
        solution_ref[1, x] = block[n, 2] * combined[0] + block[n, 3] * combined[1]


def halo_scratch(depth, fields, slots, count):
    vm = lambda *s: pltpu.VMEM(s, jnp.float32)
    dma = pltpu.SemaphoreType.DMA
    packs = -(-fields * NX // (NZ // (2 * depth)))
    return [
        vm(packs, *TILE),
        vm(slots, 2, fields, depth, *TILE), vm(slots, fields, NX, *TILE),
        vm(slots, 2, packs, *TILE), vm(slots, 2, fields, depth - 1, *TILE),
        vm(slots, 2, 2, packs, *TILE), vm(slots, 2, packs, *TILE), vm(slots, 2, 2, packs, *TILE),
        dma((count,)), dma((slots, count)),
    ]


def body(source, sigma_intra, sigma_extra, membrane):
    sizes = tuple(lax.axis_size(a) for a in AXES)
    f32 = jnp.float32
    vm = lambda *s: pltpu.VMEM(s, f32)
    dma = pltpu.SemaphoreType.DMA
    count = len(TILES)
    unscaled, remainder, scale = pl.pallas_call(
        functools.partial(cycle_kernel, sizes),
        out_shape=(vm(*source.shape), vm(*source.shape), vm(*TILE)),
        in_specs=[pl.BlockSpec(memory_space=pl.ANY)] * 4,
        out_specs=(pl.BlockSpec(memory_space=pltpu.VMEM),) * 3,
        scratch_shapes=[
            vm(KRYLOV + 1, 2, NX, *TILE), vm(2, count, 6, *TILE), vm(count, 4, *TILE), vm(NX, *TILE),
            vm(FIELDS, NX, *TILE), vm(2, NX, *TILE),
            *halo_scratch(SHALLOW, FIELDS, 1, 28), *halo_scratch(DEEP, FIELDS, 1, 28),
            *halo_scratch(SHALLOW, 2, 1, 18), *halo_scratch(DEEP, 2, 2, 26),
            vm(KRYLOV + 1, 16, NZ), vm(128, NZ), vm(3, *TILE), vm(3, 8, *TILE),
            dma((8,)), dma((3, 8)), dma((3, 8)),
        ],
        compiler_params=pltpu.CompilerParams(collective_id=0, has_side_effects=True),
    )(source, sigma_intra, sigma_extra, membrane)
    return unscaled * scale, remainder * scale


def solution(mesh):
    return jax.shard_map(
        body,
        mesh=mesh,
        in_specs=(
            P(None, "gx", "gy", "gz"),
            P(None, "gx", "gy", "gz"),
            P(None, "gx", "gy", "gz"),
            P("gx", "gy", "gz"),
        ),
        out_specs=(P(None, "gx", "gy", "gz"), P(None, "gx", "gy", "gz")),
        check_vma=False,
    )
```

```python
import functools
import itertools

import jax
import jax.numpy as jnp
from jax import lax
from jax.experimental import pallas as pl
from jax.experimental.pallas import tpu as pltpu
from jax.sharding import PartitionSpec as P

KRYLOV = 10
AXES = ("gx", "gy", "gz")
MESH = pl.DeviceIdType.MESH
NX, NY, NZ = 4, 8, 128
TILE = (NY, NZ)
OWN, BESIDE = 0, 1
FACES, EDGES, CORNERS = (
    [d for d in itertools.product((-1, 0, 1), repeat=3) if sum(abs(a) for a in d) == n]
    for n in (1, 2, 3)
)
DIRECTIONS = FACES + EDGES + CORNERS
FIELDS = 9
FIRST, DEEP = 3, 4
MEMBRANE, SOURCE = 6, 7


def tiles(reach):
    return [
        (x, ty, tz)
        for ty in (OWN, BESIDE) for tz in (OWN, BESIDE) for x in range(-reach, NX + reach)
        if max(-x, x - NX + 1, 0) + ty + tz <= reach
    ]


TILES = tiles(DEEP - 1)
PLACE = {t: n for n, t in enumerate(TILES)}


def toward(where, sizes, direction):
    return {
        AXES[a]: lax.rem(where[a] + step + sizes[a], sizes[a])
        for a, step in enumerate(direction) if step
    }


class Halo:
    def __init__(self, depth, refs, where, sizes):
        (self.own, self.pack, self.gx, self.gy, self.gz, self.gxy, self.gxz, self.gyz, self.gxyz,
         self.send_sem, self.recv_sem) = refs
        self.depth, self.stride, self.each = depth, 2 * depth, NZ // (2 * depth)
        self.where, self.sizes, self.count = where, sizes, 0

    def exists(self, direction):
        there = None
        for axis, step in enumerate(direction):
            if step:
                at = self.where[axis]
                ok = at > 0 if step < 0 else at < self.sizes[axis] - 1
                there = ok if there is None else jnp.logical_and(there, ok)
        return there

    def add(self, direction, ends):
        n = self.count
        self.count += 1

        def copy(slot):
            src, dst = ends(slot)
            return pltpu.make_async_remote_copy(
                src_ref=src, dst_ref=dst,
                send_sem=self.send_sem.at[n], recv_sem=self.recv_sem.at[slot, n],
                device_id=toward(self.where, self.sizes, direction),
                device_id_type=MESH,
            )

        return direction, copy

    def planes(self, d, fields, first, count):
        low = NX - first - count if d[0] > 0 else first
        at = self.depth - first - count if d[0] > 0 else first
        ghost = 0 if d[0] > 0 else 1
        return self.add(d, lambda slot: (
            self.own.at[fields, pl.ds(low, count)],
            self.gx.at[slot, ghost, fields, pl.ds(at, count)],
        ))

    def rows(self, d, fields, first, count):
        rows = pl.ds(NY - first - count if d[1] > 0 else first, count)
        return self.add(d, lambda slot: (
            self.own.at[fields, :, rows, :], self.gy.at[slot, fields, :, rows, :]
        ))

    def columns(self, d):
        return self.add(d, lambda slot: (self.pack, self.gz.at[slot, 0 if d[2] > 0 else 1]))

    def edge(self, d):
        dx, dy, dz = d
        ghost_x, ghost_z = (0 if dx > 0 else 1), (0 if dz > 0 else 1)
        count = self.depth - sum(abs(a) for a in d) + 1
        row = pl.ds(NY - count if dy > 0 else 0, count)
        if not dz:
            planes = pl.ds(NX - count if dx > 0 else 0, count)
            return self.add(d, lambda slot: (
                self.own.at[:, planes, row, :], self.gxy.at[slot, ghost_x, :, :, row, :]
            ))
        if not dy:
            return self.add(d, lambda slot: (self.pack, self.gxz.at[slot, ghost_x, ghost_z]))
        if not dx:
            return self.add(d, lambda slot: (
                self.pack.at[:, row, :], self.gyz.at[slot, ghost_z, :, row, :]
            ))
        return self.add(d, lambda slot: (
            self.pack.at[:, row, :], self.gxyz.at[slot, ghost_x, ghost_z, :, row, :]
        ))

    def fill_pack(self, values):
        group = lax.broadcasted_iota(jnp.int32, TILE, 1) // self.stride
        for first in range(0, len(values), self.each):
            packed = None
            for q, v in enumerate(values[first : first + self.each]):
                moved = pltpu.roll(v, self.stride * q + self.depth, 1)
                packed = moved if packed is None else jnp.where(group == q, moved, packed)
            self.pack[first // self.each] = packed

    def start(self, slot, messages):
        for d, copy in messages:
            @pl.when(self.exists(d))
            def _(copy=copy):
                copy(slot).start()

    def sent(self, slot, messages):
        for d, copy in messages:
            @pl.when(self.exists(d))
            def _(copy=copy):
                copy(slot).wait_send()

    def arrived(self, slot, messages):
        for d, copy in messages:
            @pl.when(self.exists(tuple(-a for a in d)))
            def _(copy=copy):
                copy(slot).wait_recv()

    def view(self, slot):
        return View(self, slot)


class View:
    def __init__(self, halo, slot):
        self.halo, self.slot, self.made, self.merged = halo, slot, {}, {}

    def columns(self, name, *at):
        if (name, at) not in self.merged:
            h, (*before, pack) = self.halo, at
            ref = getattr(h, name)
            low = lax.broadcasted_iota(jnp.int32, TILE, 1) % h.stride < h.depth
            self.merged[name, at] = jnp.where(
                low, ref[(self.slot, *before, 0, pack)], ref[(self.slot, *before, 1, pack)]
            )
        return self.merged[name, at]

    def tile(self, f, x, ty, tz, turn=0):
        key = (f, x, ty, tz, turn)
        if key not in self.made:
            self.made[key] = self.make(f, x, ty, tz, turn)
        return self.made[key]

    def make(self, f, x, ty, tz, turn):
        h = self.halo
        outside = (0,) if x < 0 else (1,) if x >= NX else ()
        if tz == BESIDE:
            pack, q = divmod(f * NX + x % NX, h.each)
            name = "g" + ("x" if outside else "") + ("y" if ty == BESIDE else "") + "z"
            source = self.columns(name, *outside, pack)
            return pltpu.roll(source, (turn - h.stride * q - h.depth) % NZ, 1)
        if turn:
            return pltpu.roll(self.tile(f, x, ty, tz), turn % NZ, 1)
        if ty == BESIDE:
            if not outside:
                return h.gy[self.slot, f, x]
            return h.gxy[self.slot, outside[0], f, x + h.depth - 1 if x < 0 else x - NX]
        if not outside:
            return h.own[f, x]
        return h.gx[self.slot, outside[0], f, x + h.depth if x < 0 else x - NX]


class Values:
    def __init__(self, values):
        self.values, self.made = values, {}

    def tile(self, f, x, ty, tz, turn=0):
        v = self.values[f][x, ty, tz]
        if not turn:
            return v
        key = (f, x, ty, tz, turn)
        if key not in self.made:
            self.made[key] = pltpu.roll(v, turn % NZ, 1)
        return self.made[key]


def beside(view, f, t, axis, step):
    x, ty, tz = t
    if axis == 0:
        return view.tile(f, x + step, ty, tz)
    if axis == 1:
        edge = lax.broadcasted_iota(jnp.int32, TILE, 0) == (0 if step < 0 else NY - 1)
        shift = 1 if step < 0 else NY - 1
        return jnp.where(
            edge,
            pltpu.roll(view.tile(f, x, 1 - ty, tz), shift, 0),
            pltpu.roll(view.tile(f, x, ty, tz), shift, 0),
        )
    edge = lax.broadcasted_iota(jnp.int32, TILE, 1) == (0 if step < 0 else NZ - 1)
    return jnp.where(edge, view.tile(f, x, ty, 1 - tz, -step), view.tile(f, x, ty, tz, -step))


def two_sum(a, b):
    s = a + b
    t = s - a
    return s, (a - (s - t)) + (b - t)


def add_pair(a, b):
    s, e = two_sum(a[0], b[0])
    return s, e + (a[1] + b[1])


def halves(a):
    c = 4097.0 * a
    top = c - (c - a)
    return top, a - top


def product(a, b, a_halves, b_halves):
    (ah, al), (bh, bl) = a_halves, b_halves
    p = a * b
    return p, ((ah * bh - p) + ah * bl + al * bh) + al * bl


class Pair:
    def __init__(self, high, low):
        self.high, self.low = two_sum(high, low)
        self.halves = halves(self.high)

    def times(self, other):
        p, e = product(self.high, other.high, self.halves, other.halves)
        return p, e + (self.high * other.low + self.low * other.high)


def minimizer(high, low):
    size = KRYLOV + 1
    row = lax.broadcasted_iota(jnp.int32, TILE, 0)
    col = lax.broadcasted_iota(jnp.int32, TILE, 1)
    groups = (NY + 3 - 1, 2)
    assert groups[0] == size - 1

    def column(j, group):
        i = groups[group] - row
        mask = col == lax.shift_right_arithmetic(i * (i + 1), 1) + j
        return tuple(
            jnp.broadcast_to(jnp.sum(jnp.where(mask, v, 0.0), axis=1, keepdims=True), TILE)
            for v in (high, low)
        )

    def place(i):
        return (0, groups[0] - i) if i > groups[1] else (1, groups[1] - i)

    def entry(vectors, i):
        group, r = place(i)
        return tuple(jnp.broadcast_to(v[r : r + 1, :], TILE) for v in vectors[group])

    columns = [{g: column(j, g) for g in range(2) if g == 0 or j <= groups[1]} for j in range(size)]
    first = entry(columns[0], 0)
    right = {0: first, 1: first}
    factors, solved = [], []
    for k in range(size):
        pivot = Pair(*entry(columns[k], k))
        guess = 1.0 / pivot.high
        p, e = product(pivot.high, guess, pivot.halves, halves(guess))
        inverse = Pair(guess, guess * (((1.0 - p) - e) - pivot.low * guess))
        bk = Pair(*entry(right, k))
        solved.append(sum(bk.times(inverse)))
        live = [g for g in range(2) if (g == 0 and k < size - 1) or (g == 1 and k < groups[1])]
        factor = {g: Pair(*Pair(*columns[k][g]).times(inverse)) for g in live}
        factors.append({g: (factor[g].high, factor[g].low) for g in live})
        targets = [(columns[j], Pair(*entry(columns[k], j))) for j in range(k + 1, size)]
        for target, by in targets + [(right, bk)]:
            for g in live:
                if g in target:
                    p, e = factor[g].times(by)
                    s, t = two_sum(target[g][0], -p)
                    target[g] = s, target[g][1] + (t - e)
    z = [None] * size
    for k in range(size - 1, -1, -1):
        rest = solved[k]
        for i in range(size - 1, k, -1):
            rest = rest - entry(factors[k], i)[0] * z[i]
        z[k] = rest
    return z


def cycle_kernel(
    sizes,
    source_hbm, intra_hbm, extra_hbm, membrane_hbm,
    solution_ref, residual_ref, scale_ref,
    basis, coef, block, inverse,
    s_own, u_own, *refs,
):
    groups = [refs[10 * n : 10 * n + 10] for n in range(3)]
    gram_all, mine, parts, local_sem, sum_send, sum_recv = refs[30:]
    where = [lax.axis_index(a) for a in AXES]
    s_deep = s_own.at[pl.ds(0, MEMBRANE + 1)]
    cells, deep_cells, halo = (
        Halo(depth, (own, *group), where, sizes)
        for depth, own, group in zip((FIRST, DEEP, DEEP), (s_own, s_deep, u_own), groups)
    )

    def all_messages(h, plane_sets):
        made = [h.edge(d) for d in CORNERS + EDGES]
        for d in FACES:
            if d[0]:
                made += [h.planes(d, fields, 0, count) for fields, count in plane_sets]
            elif d[1]:
                made.append(h.rows(d, slice(None), 0, h.depth))
            else:
                made.append(h.columns(d))
        return made

    first_messages = all_messages(cells, [(pl.ds(0, 2), FIRST), (pl.ds(2, 7), FIRST - 1)])
    deep_messages = all_messages(deep_cells, [(pl.ds(0, 2), DEEP), (pl.ds(2, 5), DEEP - 1)])
    messages = all_messages(halo, [(slice(None), DEEP)])

    loads = [
        pltpu.make_async_copy(ref.at[axis], s_own.at[2 * axis + s], local_sem.at[2 * axis + s])
        for axis in range(3) for s, ref in enumerate((intra_hbm, extra_hbm))
    ] + [
        pltpu.make_async_copy(membrane_hbm, s_own.at[6], local_sem.at[6]),
        pltpu.make_async_copy(source_hbm, s_own.at[pl.ds(7, 2)], local_sem.at[7]),
    ]
    for c in loads:
        c.start()
    for h in (cells, deep_cells, halo):
        for ref in (h.gx, h.gy, h.gz, h.gxy, h.gxz, h.gyz, h.gxyz):
            ref[...] = jnp.zeros_like(ref)

    barrier = pltpu.get_barrier_semaphore()
    expected = 0
    for d in DIRECTIONS:
        there = cells.exists(d)
        expected = expected + jnp.where(there, 1, 0)

        @pl.when(there)
        def _(d=d):
            pl.semaphore_signal(
                barrier, inc=1,
                device_id=toward(where, sizes, d),
                device_id_type=MESH,
            )
    for d in range(3):
        for far in range(5, sizes[d]):
            for step in (-far, far):
                there = where[d] >= far if step < 0 else where[d] < sizes[d] - far
                expected = expected + jnp.where(there, 1, 0)

                @pl.when(there)
                def _(d=d, step=step):
                    pl.semaphore_signal(
                        barrier, inc=1, device_id={AXES[d]: lax.rem(where[d] + step + sizes[d], sizes[d])}, device_id_type=MESH
                    )
    gram_all[...] = jnp.zeros_like(gram_all)
    for k in range(1, KRYLOV + 1):
        basis[k] = jnp.zeros_like(basis.at[k])
    for c in loads:
        c.wait()
    cells.fill_pack([s_own[f, x] for f in range(FIELDS) for x in range(NX)])
    pl.semaphore_wait(barrier, expected)

    cells.start(0, first_messages)
    deep_cells.fill_pack([s_own[f, x] for f in range(MEMBRANE + 1) for x in range(NX)])
    deep_cells.start(0, deep_messages)

    def coefficients(view, cells_at):
        for t in cells_at:
            n = PLACE[t]
            diagonals = []
            for s in range(2):
                total = None
                for axis in range(3):
                    here = view.tile(2 * axis + s, *t)
                    lower = 0.5 * (here + beside(view, 2 * axis + s, t, axis, -1))
                    upper = 0.5 * (here + beside(view, 2 * axis + s, t, axis, 1))
                    coef[s, n, 2 * axis] = lower
                    coef[s, n, 2 * axis + 1] = upper
                    total = upper + lower if total is None else total + upper + lower
                diagonals.append(total)
            di, de, m = diagonals[0], diagonals[1], view.tile(MEMBRANE, *t)
            det = m * di + m * de + di * de
            inside = m > 0.0
            over = jnp.where(inside, 1.0 / jnp.where(inside, det, 1.0), 0.0)
            block[n, 0] = de * over
            block[n, 1] = m * over
            block[n, 2] = -di * over
            block[n, 3] = (m + di) * over
            if t in own:
                inverse[t[0]] = (di + de) * over

    own = [(x, OWN, OWN) for x in range(NX)]
    def solved(t, a, b):
        n = PLACE[t]
        return block[n, 0] * a + block[n, 1] * b, block[n, 2] * a + block[n, 3] * b

    def apply(view, t):
        n = PLACE[t]
        off = []
        for s in range(2):
            total = None
            for axis in range(3):
                for side, step in enumerate((-1, 1)):
                    term = coef[s, n, 2 * axis + side] * beside(view, s, t, axis, step)
                    total = term if total is None else total + term
            off.append(total)
        return off[0], off[0] + off[1]

    def load(k):
        return [[basis[k, s, x] for x in range(NX)] for s in range(2)]

    def keep(k, v):
        for s in range(2):
            for x in range(NX):
                basis[k, s, x] = v[s][x]

    def stage(h, v):
        values = [[None] * NX for _ in range(2)]
        for x in range(NX):
            values[0][x], values[1][x] = solved(own[x], v[0][x], v[1][x])
        for s in range(2):
            for x in range(NX):
                u_own[s, x] = values[s][x]
        h.fill_pack(values[0] + values[1])

    def gram_row(k):
        at, first = load(k), k * (k + 1) // 2
        for i in range(k + 1):
            total = None
            for s in range(2):
                for x in range(NX):
                    term = at[s][x] * basis[i, s, x]
                    total = term if total is None else total + term
            gram_all[pl.ds(first + i, 1), :] = jnp.sum(total, axis=0, keepdims=True)

    def powers(view, depth):
        made = []
        for reach in range(depth - 1, -1, -1):
            now = {t: apply(view, t) for t in tiles(reach)}
            made.append([[now[t][s] for t in own] for s in range(2)])
            if reach:
                view = solved_at(now)
        return made

    def solved_at(pairs):
        then = {t: solved(t, *pair) for t, pair in pairs.items()}
        return Values([{t: then[t][s] for t in then} for s in range(2)])

    def combine(f, *vs):
        return [[f(*(v[s][x] for v in vs)) for x in range(NX)] for s in range(2)]

    def advance(k, view, depth):
        here = load(k)
        made = powers(view, depth)
        terms = [
            made[0],
            combine(lambda b, a: 2.0 * b - a, made[1], here),
        ]
        if depth > 2:
            terms.append(combine(lambda b, a: 4.0 * b - 3.0 * a, made[2], made[0]))
            terms.append(combine(lambda b, a, r: 8.0 * b - 8.0 * a + r, made[3], made[1], here))
        if k == 0:
            return terms
        return [
            combine(lambda t, p: 2.0 * t - p, t, load(abs(k - 1 - j))) for j, t in enumerate(terms)
        ]

    def extend(k, made):
        for j, v in enumerate(made):
            keep(k + 1 + j, v)
        for j in range(len(made)):
            gram_row(k + 1 + j)

    keep(0, [[s_own[SOURCE + s, x] for x in range(NX)] for s in range(2)])
    gram_row(0)
    cells.sent(0, first_messages)
    cells.arrived(0, first_messages)
    view = cells.view(0)
    coefficients(view, tiles(FIRST - 1))
    start = {t: [view.tile(SOURCE + s, *t) for s in range(2)] for t in tiles(FIRST - 1)}
    made = advance(0, solved_at(start), FIRST - 1)
    stage(halo, made[-1])
    halo.start(0, messages)
    extend(0, made)
    deep_cells.sent(0, deep_messages)
    deep_cells.arrived(0, deep_messages)
    complete = [(x, OWN, OWN) for x in range(1 - FIRST, NX + FIRST - 1)]
    coefficients(deep_cells.view(0), [t for t in TILES if t not in complete])
    for slot, k in enumerate((2, 6)):
        halo.sent(slot, messages)
        halo.arrived(slot, messages)
        made = advance(k, halo.view(slot), DEEP)
        if slot == 0:
            stage(halo, made[-1])
            halo.start(1, messages)
        extend(k, made)

    ones = jnp.ones(TILE, jnp.bfloat16)
    left, totals = gram_all[...], []
    for _ in range(3):
        piece = left.astype(jnp.bfloat16)
        left = left - piece.astype(jnp.float32)
        totals.append(lax.dot_general(
            ones, piece, (((1,), (1,)), ((), ())), preferred_element_type=jnp.float32
        )[0:1, :])
    high, low = two_sum(totals[0], totals[1])
    low = low + totals[2]
    for n, d in enumerate((2, 1, 0)):
        size = sizes[d]
        mine[n, 0:1, :] = high
        mine[n, 1:2, :] = low
        parts[n, where[d], 0:1, :] = high
        parts[n, where[d], 1:2, :] = low

        def copy(j, slot, other):
            return pltpu.make_async_remote_copy(
                src_ref=mine.at[n, pl.ds(0, 2), :], dst_ref=parts.at[n, slot, pl.ds(0, 2), :],
                send_sem=sum_send.at[n, j], recv_sem=sum_recv.at[n, slot],
                device_id={AXES[d]: other}, device_id_type=MESH,
            )

        others = [(j, lax.rem(where[d] + j, size)) for j in range(1, size)]
        for j, other in others:
            copy(j, where[d], other).start()
        for j, other in others:
            copy(j, other, other).wait_recv()
        for j, other in others:
            copy(j, where[d], other).wait_send()
        terms = [(parts[n, j, 0:1, :], parts[n, j, 1:2, :]) for j in range(size)]
        while len(terms) > 1:
            terms = [add_pair(terms[i], terms[i + 1]) for i in range(0, len(terms), 2)]
        high, low = two_sum(*terms[0])

    z = minimizer(jnp.broadcast_to(high, TILE), jnp.broadcast_to(low, TILE))
    size = KRYLOV + 1
    total = z[0]
    for k in range(1, size):
        total = total + z[k]
    scale_ref[...] = 1.0 / total
    rho = z
    slope = [None] * size
    running = jnp.zeros(TILE, jnp.float32)
    weighted = jnp.zeros(TILE, jnp.float32)
    for j in range(KRYLOV - 1, -1, -1):
        running = running + rho[j + 1]
        weighted = weighted + running
        slope[j] = weighted
    coeffs = [slope[0]] + [2.0 * slope[j] for j in range(1, KRYLOV)]

    for x in range(NX):
        combined = []
        for s in range(2):
            vectors = [basis[k, s, x] for k in range(size)]
            r = rho[0] * vectors[0]
            c = coeffs[0] * vectors[0]
            for k in range(1, size):
                r = r + rho[k] * vectors[k]
                if k < KRYLOV:
                    c = c + coeffs[k] * vectors[k]
            residual_ref[s, x] = r
            combined.append(c)
        n = PLACE[own[x]]
        solution_ref[0, x] = inverse[x] * combined[0] + block[n, 2] * combined[1]
        solution_ref[1, x] = block[n, 2] * combined[0] + block[n, 3] * combined[1]


def halo_scratch(depth, fields, slots, count):
    vm = lambda *s: pltpu.VMEM(s, jnp.float32)
    dma = pltpu.SemaphoreType.DMA
    packs = -(-fields * NX // (NZ // (2 * depth)))
    return [
        vm(packs, *TILE),
        vm(slots, 2, fields, depth, *TILE), vm(slots, fields, NX, *TILE),
        vm(slots, 2, packs, *TILE), vm(slots, 2, fields, depth - 1, *TILE),
        vm(slots, 2, 2, packs, *TILE), vm(slots, 2, packs, *TILE), vm(slots, 2, 2, packs, *TILE),
        dma((count,)), dma((slots, count)),
    ]


def body(source, sigma_intra, sigma_extra, membrane):
    sizes = tuple(lax.axis_size(a) for a in AXES)
    f32 = jnp.float32
    vm = lambda *s: pltpu.VMEM(s, f32)
    dma = pltpu.SemaphoreType.DMA
    count = len(TILES)
    unscaled, remainder, scale = pl.pallas_call(
        functools.partial(cycle_kernel, sizes),
        out_shape=(vm(*source.shape), vm(*source.shape), vm(*TILE)),
        in_specs=[pl.BlockSpec(memory_space=pl.ANY)] * 4,
        out_specs=(pl.BlockSpec(memory_space=pltpu.VMEM),) * 3,
        scratch_shapes=[
            vm(KRYLOV + 1, 2, NX, *TILE), vm(2, count, 6, *TILE), vm(count, 4, *TILE), vm(NX, *TILE),
            vm(FIELDS, NX, *TILE), vm(2, NX, *TILE),
            *halo_scratch(FIRST, FIELDS, 1, 28), *halo_scratch(DEEP, MEMBRANE + 1, 1, 28),
            *halo_scratch(DEEP, 2, 2, 26),
            vm(128, NZ), vm(3, *TILE), vm(3, 8, *TILE),
            dma((8,)), dma((3, 8)), dma((3, 8)),
        ],
        compiler_params=pltpu.CompilerParams(collective_id=0, has_side_effects=True),
    )(source, sigma_intra, sigma_extra, membrane)
    return unscaled * scale, remainder * scale


def solution(mesh):
    return jax.shard_map(
        body,
        mesh=mesh,
        in_specs=(
            P(None, "gx", "gy", "gz"),
            P(None, "gx", "gy", "gz"),
            P(None, "gx", "gy", "gz"),
            P("gx", "gy", "gz"),
        ),
        out_specs=(P(None, "gx", "gy", "gz"), P(None, "gx", "gy", "gz")),
        check_vma=False,
    )
```

```python
import functools
import itertools

import jax
import jax.numpy as jnp
from jax import lax
from jax.experimental import pallas as pl
from jax.experimental.pallas import tpu as pltpu
from jax.sharding import PartitionSpec as P

KRYLOV = 10
AXES = ("gx", "gy", "gz")
MESH = pl.DeviceIdType.MESH
NX, NY, NZ = 4, 8, 128
TILE = (NY, NZ)
OWN, BESIDE = 0, 1
FACES, EDGES, CORNERS = (
    [d for d in itertools.product((-1, 0, 1), repeat=3) if sum(abs(a) for a in d) == n]
    for n in (1, 2, 3)
)
DIRECTIONS = FACES + EDGES + CORNERS
FIELDS = 9
FIRST, DEEP = 3, 4
MEMBRANE, SOURCE = 6, 7


def tiles(reach):
    return [
        (x, ty, tz)
        for ty in (OWN, BESIDE) for tz in (OWN, BESIDE) for x in range(-reach, NX + reach)
        if max(-x, x - NX + 1, 0) + ty + tz <= reach
    ]


TILES = tiles(DEEP - 1)
PLACE = {t: n for n, t in enumerate(TILES)}


def toward(where, sizes, direction):
    return {
        AXES[a]: lax.rem(where[a] + step + sizes[a], sizes[a])
        for a, step in enumerate(direction) if step
    }


class Halo:
    def __init__(self, depth, refs, where, sizes):
        (self.own, self.pack, self.gx, self.gy, self.gz, self.gxy, self.gxz, self.gyz, self.gxyz,
         self.send_sem, self.recv_sem) = refs
        self.depth, self.stride, self.each = depth, 2 * depth, NZ // (2 * depth)
        self.where, self.sizes, self.count = where, sizes, 0

    def exists(self, direction):
        there = None
        for axis, step in enumerate(direction):
            if step:
                at = self.where[axis]
                ok = at > 0 if step < 0 else at < self.sizes[axis] - 1
                there = ok if there is None else jnp.logical_and(there, ok)
        return there

    def add(self, direction, ends):
        n = self.count
        self.count += 1

        def copy(slot):
            src, dst = ends(slot)
            return pltpu.make_async_remote_copy(
                src_ref=src, dst_ref=dst,
                send_sem=self.send_sem.at[n], recv_sem=self.recv_sem.at[slot, n],
                device_id=toward(self.where, self.sizes, direction),
                device_id_type=MESH,
            )

        return direction, copy

    def planes(self, d, fields, first, count):
        low = NX - first - count if d[0] > 0 else first
        at = DEEP - first - count if d[0] > 0 else first
        ghost = 0 if d[0] > 0 else 1
        return self.add(d, lambda slot: (
            self.own.at[fields, pl.ds(low, count)],
            self.gx.at[slot, ghost, fields, pl.ds(at, count)],
        ))

    def rows(self, d, fields, first, count):
        rows = pl.ds(NY - first - count if d[1] > 0 else first, count)
        return self.add(d, lambda slot: (
            self.own.at[fields, :, rows, :], self.gy.at[slot, fields, :, rows, :]
        ))

    def columns(self, d):
        return self.add(d, lambda slot: (self.pack, self.gz.at[slot, 0 if d[2] > 0 else 1]))

    def corner_rows(self, d, fields, count):
        planes = pl.ds(NX - count if d[0] > 0 else 0, count)
        at = pl.ds(self.depth - 1 - count if d[0] > 0 else 0, count)
        row = pl.ds(NY - count if d[1] > 0 else 0, count)
        ghost = 0 if d[0] > 0 else 1
        return self.add(d, lambda slot: (
            self.own.at[fields, planes, row, :], self.gxy.at[slot, ghost, fields, at, row, :]
        ))

    def edge(self, d):
        dx, dy, dz = d
        ghost_x, ghost_z = (0 if dx > 0 else 1), (0 if dz > 0 else 1)
        count = self.depth - sum(abs(a) for a in d) + 1
        row = pl.ds(NY - count if dy > 0 else 0, count)
        if not dy:
            return self.add(d, lambda slot: (self.pack, self.gxz.at[slot, ghost_x, ghost_z]))
        if not dx:
            return self.add(d, lambda slot: (
                self.pack.at[:, row, :], self.gyz.at[slot, ghost_z, :, row, :]
            ))
        return self.add(d, lambda slot: (
            self.pack.at[:, row, :], self.gxyz.at[slot, ghost_x, ghost_z, :, row, :]
        ))

    def fill_pack(self, values):
        group = lax.broadcasted_iota(jnp.int32, TILE, 1) // self.stride
        for first in range(0, len(values), self.each):
            packed = None
            for q, v in enumerate(values[first : first + self.each]):
                moved = pltpu.roll(v, self.stride * q + self.depth, 1)
                packed = moved if packed is None else jnp.where(group == q, moved, packed)
            self.pack[first // self.each] = packed

    def start(self, slot, messages):
        for d, copy in messages:
            @pl.when(self.exists(d))
            def _(copy=copy):
                copy(slot).start()

    def sent(self, slot, messages):
        for d, copy in messages:
            @pl.when(self.exists(d))
            def _(copy=copy):
                copy(slot).wait_send()

    def arrived(self, slot, messages):
        for d, copy in messages:
            @pl.when(self.exists(tuple(-a for a in d)))
            def _(copy=copy):
                copy(slot).wait_recv()

    def view(self, slot):
        return View(self, slot)


class View:
    def __init__(self, halo, slot):
        self.halo, self.slot, self.made, self.merged = halo, slot, {}, {}

    def columns(self, name, *at):
        if (name, at) not in self.merged:
            h, (*before, pack) = self.halo, at
            ref = getattr(h, name)
            low = lax.broadcasted_iota(jnp.int32, TILE, 1) % h.stride < h.depth
            self.merged[name, at] = jnp.where(
                low, ref[(self.slot, *before, 0, pack)], ref[(self.slot, *before, 1, pack)]
            )
        return self.merged[name, at]

    def tile(self, f, x, ty, tz, turn=0):
        key = (f, x, ty, tz, turn)
        if key not in self.made:
            self.made[key] = self.make(f, x, ty, tz, turn)
        return self.made[key]

    def make(self, f, x, ty, tz, turn):
        h = self.halo
        outside = (0,) if x < 0 else (1,) if x >= NX else ()
        if tz == BESIDE:
            pack, q = divmod(f * NX + x % NX, h.each)
            name = "g" + ("x" if outside else "") + ("y" if ty == BESIDE else "") + "z"
            source = self.columns(name, *outside, pack)
            return pltpu.roll(source, (turn - h.stride * q - h.depth) % NZ, 1)
        if turn:
            return pltpu.roll(self.tile(f, x, ty, tz), turn % NZ, 1)
        if ty == BESIDE:
            if not outside:
                return h.gy[self.slot, f, x]
            return h.gxy[self.slot, outside[0], f, x + h.depth - 1 if x < 0 else x - NX]
        if not outside:
            return h.own[f, x]
        return h.gx[self.slot, outside[0], f, x + DEEP if x < 0 else x - NX]


class Values:
    def __init__(self, values):
        self.values, self.made = values, {}

    def tile(self, f, x, ty, tz, turn=0):
        v = self.values[f][x, ty, tz]
        if not turn:
            return v
        key = (f, x, ty, tz, turn)
        if key not in self.made:
            self.made[key] = pltpu.roll(v, turn % NZ, 1)
        return self.made[key]


def beside(view, f, t, axis, step):
    x, ty, tz = t
    if axis == 0:
        return view.tile(f, x + step, ty, tz)
    if axis == 1:
        edge = lax.broadcasted_iota(jnp.int32, TILE, 0) == (0 if step < 0 else NY - 1)
        shift = 1 if step < 0 else NY - 1
        return jnp.where(
            edge,
            pltpu.roll(view.tile(f, x, 1 - ty, tz), shift, 0),
            pltpu.roll(view.tile(f, x, ty, tz), shift, 0),
        )
    edge = lax.broadcasted_iota(jnp.int32, TILE, 1) == (0 if step < 0 else NZ - 1)
    return jnp.where(edge, view.tile(f, x, ty, 1 - tz, -step), view.tile(f, x, ty, tz, -step))


def two_sum(a, b):
    s = a + b
    t = s - a
    return s, (a - (s - t)) + (b - t)


def add_pair(a, b):
    s, e = two_sum(a[0], b[0])
    return s, e + (a[1] + b[1])


def halves(a):
    c = 4097.0 * a
    top = c - (c - a)
    return top, a - top


def product(a, b, a_halves, b_halves):
    (ah, al), (bh, bl) = a_halves, b_halves
    p = a * b
    return p, ((ah * bh - p) + ah * bl + al * bh) + al * bl


class Pair:
    def __init__(self, high, low):
        self.high, self.low = two_sum(high, low)
        self.halves = halves(self.high)

    def times(self, other):
        p, e = product(self.high, other.high, self.halves, other.halves)
        return p, e + (self.high * other.low + self.low * other.high)


def minimizer(high, low):
    size = KRYLOV + 1
    row = lax.broadcasted_iota(jnp.int32, TILE, 0)
    col = lax.broadcasted_iota(jnp.int32, TILE, 1)
    groups = (NY + 3 - 1, 2)
    assert groups[0] == size - 1

    def column(j, group):
        i = groups[group] - row
        mask = col == lax.shift_right_arithmetic(i * (i + 1), 1) + j
        return tuple(
            jnp.broadcast_to(jnp.sum(jnp.where(mask, v, 0.0), axis=1, keepdims=True), TILE)
            for v in (high, low)
        )

    def place(i):
        return (0, groups[0] - i) if i > groups[1] else (1, groups[1] - i)

    def entry(vectors, i):
        group, r = place(i)
        return tuple(jnp.broadcast_to(v[r : r + 1, :], TILE) for v in vectors[group])

    columns = [{g: column(j, g) for g in range(2) if g == 0 or j <= groups[1]} for j in range(size)]
    first = entry(columns[0], 0)
    right = {0: first, 1: first}
    factors, solved = [], []
    for k in range(size):
        pivot = Pair(*entry(columns[k], k))
        guess = 1.0 / pivot.high
        p, e = product(pivot.high, guess, pivot.halves, halves(guess))
        inverse = Pair(guess, guess * (((1.0 - p) - e) - pivot.low * guess))
        bk = Pair(*entry(right, k))
        solved.append(sum(bk.times(inverse)))
        live = [g for g in range(2) if (g == 0 and k < size - 1) or (g == 1 and k < groups[1])]
        factor = {g: Pair(*Pair(*columns[k][g]).times(inverse)) for g in live}
        factors.append({g: (factor[g].high, factor[g].low) for g in live})
        targets = [(columns[j], Pair(*entry(columns[k], j))) for j in range(k + 1, size)]
        for target, by in targets + [(right, bk)]:
            for g in live:
                if g in target:
                    p, e = factor[g].times(by)
                    s, t = two_sum(target[g][0], -p)
                    target[g] = s, target[g][1] + (t - e)
    z = [None] * size
    for k in range(size - 1, -1, -1):
        rest = solved[k]
        for i in range(size - 1, k, -1):
            rest = rest - entry(factors[k], i)[0] * z[i]
        z[k] = rest
    return z


def cycle_kernel(
    sizes,
    source_hbm, intra_hbm, extra_hbm, membrane_hbm,
    solution_ref, residual_ref, scale_ref,
    basis, coef, block, inverse,
    s_own, u_own, *refs,
):
    groups = [refs[10 * n : 10 * n + 10] for n in range(3)]
    gram_all, mine, parts, local_sem, sum_send, sum_recv = refs[30:]
    where = [lax.axis_index(a) for a in AXES]
    s_deep = s_own.at[pl.ds(0, MEMBRANE + 1)]
    cells, deep_cells, halo = (
        Halo(depth, (own, *group), where, sizes)
        for depth, own, group in zip((FIRST, DEEP, DEEP), (s_own, s_deep, u_own), groups)
    )

    deep_cells.gx = cells.gx

    def all_messages(h, plane_sets, row_sets):
        made = [h.edge(d) for d in CORNERS]
        for d in EDGES:
            if d[2]:
                made.append(h.edge(d))
            else:
                made += [h.corner_rows(d, *fields) for fields in row_sets]
        for d in FACES:
            if d[0]:
                made += [h.planes(d, *planes) for planes in plane_sets]
            elif d[1]:
                made.append(h.rows(d, slice(None), 0, h.depth))
            else:
                made.append(h.columns(d))
        return made

    first_messages = all_messages(cells, [
        (pl.ds(0, 2), 0, FIRST), (pl.ds(2, 7), 0, FIRST - 1),
    ], [(pl.ds(0, 4), FIRST - 1), (pl.ds(4, 5), FIRST - 2)])
    deep_messages = all_messages(deep_cells, [
        (pl.ds(0, 2), FIRST, 1), (pl.ds(2, 5), FIRST - 1, 1),
    ], [(pl.ds(0, 4), DEEP - 1), (pl.ds(4, 3), DEEP - 2)])
    messages = all_messages(halo, [(slice(None), 0, DEEP)], [(slice(None), DEEP - 1)])

    loads = [
        pltpu.make_async_copy(ref.at[axis], s_own.at[2 * axis + s], local_sem.at[2 * axis + s])
        for axis in range(3) for s, ref in enumerate((intra_hbm, extra_hbm))
    ] + [
        pltpu.make_async_copy(membrane_hbm, s_own.at[6], local_sem.at[6]),
        pltpu.make_async_copy(source_hbm, s_own.at[pl.ds(7, 2)], local_sem.at[7]),
    ]
    for c in loads:
        c.start()
    for h in (cells, deep_cells, halo):
        for ref in (h.gx, h.gy, h.gz, h.gxy, h.gxz, h.gyz, h.gxyz):
            ref[...] = jnp.zeros_like(ref)

    barrier = pltpu.get_barrier_semaphore()
    expected = 0
    for d in DIRECTIONS:
        there = cells.exists(d)
        expected = expected + jnp.where(there, 1, 0)

        @pl.when(there)
        def _(d=d):
            pl.semaphore_signal(
                barrier, inc=1,
                device_id=toward(where, sizes, d),
                device_id_type=MESH,
            )
    for d in range(3):
        for far in range(5, sizes[d]):
            for step in (-far, far):
                there = where[d] >= far if step < 0 else where[d] < sizes[d] - far
                expected = expected + jnp.where(there, 1, 0)

                @pl.when(there)
                def _(d=d, step=step):
                    pl.semaphore_signal(
                        barrier, inc=1, device_id={AXES[d]: lax.rem(where[d] + step + sizes[d], sizes[d])}, device_id_type=MESH
                    )
    gram_all[...] = jnp.zeros_like(gram_all)
    for k in range(1, KRYLOV + 1):
        basis[k] = jnp.zeros_like(basis.at[k])
    for c in loads:
        c.wait()
    cells.fill_pack([s_own[f, x] for f in range(FIELDS) for x in range(NX)])
    pl.semaphore_wait(barrier, expected)

    cells.start(0, first_messages)
    deep_cells.fill_pack([s_own[f, x] for f in range(MEMBRANE + 1) for x in range(NX)])
    deep_cells.start(0, deep_messages)

    def coefficients(view, cells_at):
        for t in cells_at:
            n = PLACE[t]
            diagonals = []
            for s in range(2):
                total = None
                for axis in range(3):
                    here = view.tile(2 * axis + s, *t)
                    lower = 0.5 * (here + beside(view, 2 * axis + s, t, axis, -1))
                    upper = 0.5 * (here + beside(view, 2 * axis + s, t, axis, 1))
                    coef[s, n, 2 * axis] = lower
                    coef[s, n, 2 * axis + 1] = upper
                    total = upper + lower if total is None else total + upper + lower
                diagonals.append(total)
            di, de, m = diagonals[0], diagonals[1], view.tile(MEMBRANE, *t)
            det = m * di + m * de + di * de
            inside = m > 0.0
            over = jnp.where(inside, 1.0 / jnp.where(inside, det, 1.0), 0.0)
            block[n, 0] = de * over
            block[n, 1] = m * over
            block[n, 2] = -di * over
            block[n, 3] = (m + di) * over
            if t in own:
                inverse[t[0]] = (di + de) * over

    own = [(x, OWN, OWN) for x in range(NX)]
    def solved(t, a, b):
        n = PLACE[t]
        return block[n, 0] * a + block[n, 1] * b, block[n, 2] * a + block[n, 3] * b

    def apply(view, t):
        n = PLACE[t]
        off = []
        for s in range(2):
            total = None
            for axis in range(3):
                for side, step in enumerate((-1, 1)):
                    term = coef[s, n, 2 * axis + side] * beside(view, s, t, axis, step)
                    total = term if total is None else total + term
            off.append(total)
        return off[0], off[0] + off[1]

    def load(k):
        return [[basis[k, s, x] for x in range(NX)] for s in range(2)]

    def keep(k, v):
        for s in range(2):
            for x in range(NX):
                basis[k, s, x] = v[s][x]

    def stage(h, v):
        values = [[None] * NX for _ in range(2)]
        for x in range(NX):
            values[0][x], values[1][x] = solved(own[x], v[0][x], v[1][x])
        for s in range(2):
            for x in range(NX):
                u_own[s, x] = values[s][x]
        h.fill_pack(values[0] + values[1])

    def gram_row(k):
        at, first = load(k), k * (k + 1) // 2
        for i in range(k + 1):
            total = None
            for s in range(2):
                for x in range(NX):
                    term = at[s][x] * basis[i, s, x]
                    total = term if total is None else total + term
            gram_all[pl.ds(first + i, 1), :] = jnp.sum(total, axis=0, keepdims=True)

    def powers(view, depth):
        made = []
        for reach in range(depth - 1, -1, -1):
            now = {t: apply(view, t) for t in tiles(reach)}
            made.append([[now[t][s] for t in own] for s in range(2)])
            if reach:
                view = solved_at(now)
        return made

    def solved_at(pairs):
        then = {t: solved(t, *pair) for t, pair in pairs.items()}
        return Values([{t: then[t][s] for t in then} for s in range(2)])

    def combine(f, *vs):
        return [[f(*(v[s][x] for v in vs)) for x in range(NX)] for s in range(2)]

    def advance(k, view, depth):
        here = load(k)
        made = powers(view, depth)
        terms = [
            made[0],
            combine(lambda b, a: 2.0 * b - a, made[1], here),
        ]
        if depth > 2:
            terms.append(combine(lambda b, a: 4.0 * b - 3.0 * a, made[2], made[0]))
            terms.append(combine(lambda b, a, r: 8.0 * b - 8.0 * a + r, made[3], made[1], here))
        if k == 0:
            return terms
        return [
            combine(lambda t, p: 2.0 * t - p, t, load(abs(k - 1 - j))) for j, t in enumerate(terms)
        ]

    def extend(k, made):
        for j, v in enumerate(made):
            keep(k + 1 + j, v)
        for j in range(len(made)):
            gram_row(k + 1 + j)

    keep(0, [[s_own[SOURCE + s, x] for x in range(NX)] for s in range(2)])
    gram_row(0)
    cells.sent(0, first_messages)
    cells.arrived(0, first_messages)
    view = cells.view(0)
    coefficients(view, tiles(FIRST - 1))
    start = {t: [view.tile(SOURCE + s, *t) for s in range(2)] for t in tiles(FIRST - 1)}
    made = advance(0, solved_at(start), FIRST - 1)
    stage(halo, made[-1])
    halo.start(0, messages)
    extend(0, made)
    deep_cells.sent(0, deep_messages)
    deep_cells.arrived(0, deep_messages)
    complete = [(x, OWN, OWN) for x in range(1 - FIRST, NX + FIRST - 1)]
    coefficients(deep_cells.view(0), [t for t in TILES if t not in complete])
    for slot, k in enumerate((2, 6)):
        halo.sent(slot, messages)
        halo.arrived(slot, messages)
        made = advance(k, halo.view(slot), DEEP)
        if slot == 0:
            stage(halo, made[-1])
            halo.start(1, messages)
        extend(k, made)

    ones = jnp.ones(TILE, jnp.bfloat16)
    left, totals = gram_all[...], []
    for _ in range(3):
        piece = left.astype(jnp.bfloat16)
        left = left - piece.astype(jnp.float32)
        totals.append(lax.dot_general(
            ones, piece, (((1,), (1,)), ((), ())), preferred_element_type=jnp.float32
        )[0:1, :])
    high, low = two_sum(totals[0], totals[1])
    low = low + totals[2]
    for n, d in enumerate((2, 1, 0)):
        size = sizes[d]
        mine[n, 0:1, :] = high
        mine[n, 1:2, :] = low
        parts[n, where[d], 0:1, :] = high
        parts[n, where[d], 1:2, :] = low

        def copy(j, slot, other):
            return pltpu.make_async_remote_copy(
                src_ref=mine.at[n, pl.ds(0, 2), :], dst_ref=parts.at[n, slot, pl.ds(0, 2), :],
                send_sem=sum_send.at[n, j], recv_sem=sum_recv.at[n, slot],
                device_id={AXES[d]: other}, device_id_type=MESH,
            )

        others = [(j, lax.rem(where[d] + j, size)) for j in range(1, size)]
        for j, other in others:
            copy(j, where[d], other).start()
        for j, other in others:
            copy(j, other, other).wait_recv()
        for j, other in others:
            copy(j, where[d], other).wait_send()
        terms = [(parts[n, j, 0:1, :], parts[n, j, 1:2, :]) for j in range(size)]
        while len(terms) > 1:
            terms = [add_pair(terms[i], terms[i + 1]) for i in range(0, len(terms), 2)]
        high, low = two_sum(*terms[0])

    z = minimizer(jnp.broadcast_to(high, TILE), jnp.broadcast_to(low, TILE))
    size = KRYLOV + 1
    total = z[0]
    for k in range(1, size):
        total = total + z[k]
    scale_ref[...] = 1.0 / total
    rho = z
    slope = [None] * size
    running = jnp.zeros(TILE, jnp.float32)
    weighted = jnp.zeros(TILE, jnp.float32)
    for j in range(KRYLOV - 1, -1, -1):
        running = running + rho[j + 1]
        weighted = weighted + running
        slope[j] = weighted
    coeffs = [slope[0]] + [2.0 * slope[j] for j in range(1, KRYLOV)]

    for x in range(NX):
        combined = []
        for s in range(2):
            vectors = [basis[k, s, x] for k in range(size)]
            r = rho[0] * vectors[0]
            c = coeffs[0] * vectors[0]
            for k in range(1, size):
                r = r + rho[k] * vectors[k]
                if k < KRYLOV:
                    c = c + coeffs[k] * vectors[k]
            residual_ref[s, x] = r
            combined.append(c)
        n = PLACE[own[x]]
        solution_ref[0, x] = inverse[x] * combined[0] + block[n, 2] * combined[1]
        solution_ref[1, x] = block[n, 2] * combined[0] + block[n, 3] * combined[1]


def halo_scratch(depth, fields, slots, count):
    vm = lambda *s: pltpu.VMEM(s, jnp.float32)
    dma = pltpu.SemaphoreType.DMA
    packs = -(-fields * NX // (NZ // (2 * depth)))
    return [
        vm(packs, *TILE),
        vm(slots, 2, fields, DEEP, *TILE), vm(slots, fields, NX, *TILE),
        vm(slots, 2, packs, *TILE), vm(slots, 2, fields, depth - 1, *TILE),
        vm(slots, 2, 2, packs, *TILE), vm(slots, 2, packs, *TILE), vm(slots, 2, 2, packs, *TILE),
        dma((count,)), dma((slots, count)),
    ]


def body(source, sigma_intra, sigma_extra, membrane):
    sizes = tuple(lax.axis_size(a) for a in AXES)
    f32 = jnp.float32
    vm = lambda *s: pltpu.VMEM(s, f32)
    dma = pltpu.SemaphoreType.DMA
    count = len(TILES)
    unscaled, remainder, scale = pl.pallas_call(
        functools.partial(cycle_kernel, sizes),
        out_shape=(vm(*source.shape), vm(*source.shape), vm(*TILE)),
        in_specs=[pl.BlockSpec(memory_space=pl.ANY)] * 4,
        out_specs=(pl.BlockSpec(memory_space=pltpu.VMEM),) * 3,
        scratch_shapes=[
            vm(KRYLOV + 1, 2, NX, *TILE), vm(2, count, 6, *TILE), vm(count, 4, *TILE), vm(NX, *TILE),
            vm(FIELDS, NX, *TILE), vm(2, NX, *TILE),
            *halo_scratch(FIRST, FIELDS, 1, 32), *halo_scratch(DEEP, MEMBRANE + 1, 1, 32),
            *halo_scratch(DEEP, 2, 2, 26),
            vm(128, NZ), vm(3, *TILE), vm(3, 8, *TILE),
            dma((8,)), dma((3, 8)), dma((3, 8)),
        ],
        compiler_params=pltpu.CompilerParams(collective_id=0, has_side_effects=True),
    )(source, sigma_intra, sigma_extra, membrane)
    return unscaled * scale, remainder * scale


def solution(mesh):
    return jax.shard_map(
        body,
        mesh=mesh,
        in_specs=(
            P(None, "gx", "gy", "gz"),
            P(None, "gx", "gy", "gz"),
            P(None, "gx", "gy", "gz"),
            P("gx", "gy", "gz"),
        ),
        out_specs=(P(None, "gx", "gy", "gz"), P(None, "gx", "gy", "gz")),
        check_vma=False,
    )
```

```python
import functools
import itertools

import jax
import jax.numpy as jnp
from jax import lax
from jax.experimental import pallas as pl
from jax.experimental.pallas import tpu as pltpu
from jax.sharding import PartitionSpec as P

KRYLOV = 10
AXES = ("gx", "gy", "gz")
MESH = pl.DeviceIdType.MESH
NX, NY, NZ = 4, 8, 128
TILE = (NY, NZ)
OWN, BESIDE = 0, 1
FACES, EDGES, CORNERS = (
    [d for d in itertools.product((-1, 0, 1), repeat=3) if sum(abs(a) for a in d) == n]
    for n in (1, 2, 3)
)
DIRECTIONS = FACES + EDGES + CORNERS
FIELDS = 9
FIRST, DEEP = 3, 4
MEMBRANE, SOURCE = 6, 7


def tiles(reach):
    return [
        (x, ty, tz)
        for ty in (OWN, BESIDE) for tz in (OWN, BESIDE) for x in range(-reach, NX + reach)
        if max(-x, x - NX + 1, 0) + ty + tz <= reach
    ]


TILES = tiles(DEEP - 1)
PLACE = {t: n for n, t in enumerate(TILES)}


def toward(where, sizes, direction):
    return {
        AXES[a]: lax.rem(where[a] + step + sizes[a], sizes[a])
        for a, step in enumerate(direction) if step
    }


class Halo:
    def __init__(self, depth, refs, where, sizes):
        (self.own, self.pack, self.gx, self.gy, self.gz, self.gxy, self.gxz, self.gyz, self.gxyz,
         self.send_sem, self.recv_sem) = refs
        self.depth, self.stride, self.each = depth, 2 * depth, NZ // (2 * depth)
        self.where, self.sizes, self.count = where, sizes, 0

    def exists(self, direction):
        there = None
        for axis, step in enumerate(direction):
            if step:
                at = self.where[axis]
                ok = at > 0 if step < 0 else at < self.sizes[axis] - 1
                there = ok if there is None else jnp.logical_and(there, ok)
        return there

    def add(self, direction, ends):
        n = self.count
        self.count += 1

        def copy(slot):
            src, dst = ends(slot)
            return pltpu.make_async_remote_copy(
                src_ref=src, dst_ref=dst,
                send_sem=self.send_sem.at[n], recv_sem=self.recv_sem.at[slot, n],
                device_id=toward(self.where, self.sizes, direction),
                device_id_type=MESH,
            )

        return direction, copy

    def planes(self, d, fields, first, count):
        low = NX - first - count if d[0] > 0 else first
        at = DEEP - first - count if d[0] > 0 else first
        ghost = 0 if d[0] > 0 else 1
        return self.add(d, lambda slot: (
            self.own.at[fields, pl.ds(low, count)],
            self.gx.at[slot, ghost, fields, pl.ds(at, count)],
        ))

    def rows(self, d, fields, first, count):
        rows = pl.ds(NY - first - count if d[1] > 0 else first, count)
        return self.add(d, lambda slot: (
            self.own.at[fields, :, rows, :], self.gy.at[slot, fields, :, rows, :]
        ))

    def columns(self, d):
        return self.add(d, lambda slot: (self.pack, self.gz.at[slot, 0 if d[2] > 0 else 1]))

    def corner_rows(self, d, fields, count):
        planes = pl.ds(NX - count if d[0] > 0 else 0, count)
        at = pl.ds(self.depth - 1 - count if d[0] > 0 else 0, count)
        row = pl.ds(NY - count if d[1] > 0 else 0, count)
        ghost = 0 if d[0] > 0 else 1
        return self.add(d, lambda slot: (
            self.own.at[fields, planes, row, :], self.gxy.at[slot, ghost, fields, at, row, :]
        ))

    def edge(self, d):
        dx, dy, dz = d
        ghost_x, ghost_z = (0 if dx > 0 else 1), (0 if dz > 0 else 1)
        count = self.depth - sum(abs(a) for a in d) + 1
        row = pl.ds(NY - count if dy > 0 else 0, count)
        if not dy:
            return self.add(d, lambda slot: (self.pack, self.gxz.at[slot, ghost_x, ghost_z]))
        if not dx:
            return self.add(d, lambda slot: (
                self.pack.at[:, row, :], self.gyz.at[slot, ghost_z, :, row, :]
            ))
        return self.add(d, lambda slot: (
            self.pack.at[:, row, :], self.gxyz.at[slot, ghost_x, ghost_z, :, row, :]
        ))

    def fill_pack(self, values):
        group = lax.broadcasted_iota(jnp.int32, TILE, 1) // self.stride
        for first in range(0, len(values), self.each):
            packed = None
            for q, v in enumerate(values[first : first + self.each]):
                moved = pltpu.roll(v, self.stride * q + self.depth, 1)
                packed = moved if packed is None else jnp.where(group == q, moved, packed)
            self.pack[first // self.each] = packed

    def start(self, slot, messages):
        for d, copy in messages:
            @pl.when(self.exists(d))
            def _(copy=copy):
                copy(slot).start()

    def sent(self, slot, messages):
        for d, copy in messages:
            @pl.when(self.exists(d))
            def _(copy=copy):
                copy(slot).wait_send()

    def arrived(self, slot, messages):
        for d, copy in messages:
            @pl.when(self.exists(tuple(-a for a in d)))
            def _(copy=copy):
                copy(slot).wait_recv()

    def view(self, slot):
        return View(self, slot)


class View:
    def __init__(self, halo, slot):
        self.halo, self.slot, self.made, self.merged = halo, slot, {}, {}

    def columns(self, name, *at):
        if (name, at) not in self.merged:
            h, (*before, pack) = self.halo, at
            ref = getattr(h, name)
            low = lax.broadcasted_iota(jnp.int32, TILE, 1) % h.stride < h.depth
            self.merged[name, at] = jnp.where(
                low, ref[(self.slot, *before, 0, pack)], ref[(self.slot, *before, 1, pack)]
            )
        return self.merged[name, at]

    def tile(self, f, x, ty, tz, turn=0):
        key = (f, x, ty, tz, turn)
        if key not in self.made:
            self.made[key] = self.make(f, x, ty, tz, turn)
        return self.made[key]

    def make(self, f, x, ty, tz, turn):
        h = self.halo
        outside = (0,) if x < 0 else (1,) if x >= NX else ()
        if tz == BESIDE:
            pack, q = divmod(f * NX + x % NX, h.each)
            name = "g" + ("x" if outside else "") + ("y" if ty == BESIDE else "") + "z"
            source = self.columns(name, *outside, pack)
            return pltpu.roll(source, (turn - h.stride * q - h.depth) % NZ, 1)
        if turn:
            return pltpu.roll(self.tile(f, x, ty, tz), turn % NZ, 1)
        if ty == BESIDE:
            if not outside:
                return h.gy[self.slot, f, x]
            return h.gxy[self.slot, outside[0], f, x + h.depth - 1 if x < 0 else x - NX]
        if not outside:
            return h.own[f, x]
        return h.gx[self.slot, outside[0], f, x + DEEP if x < 0 else x - NX]


class Values:
    def __init__(self, values):
        self.values, self.made = values, {}

    def tile(self, f, x, ty, tz, turn=0):
        v = self.values[f][x, ty, tz]
        if not turn:
            return v
        key = (f, x, ty, tz, turn)
        if key not in self.made:
            self.made[key] = pltpu.roll(v, turn % NZ, 1)
        return self.made[key]


def beside(view, f, t, axis, step):
    x, ty, tz = t
    if axis == 0:
        return view.tile(f, x + step, ty, tz)
    if axis == 1:
        edge = lax.broadcasted_iota(jnp.int32, TILE, 0) == (0 if step < 0 else NY - 1)
        shift = 1 if step < 0 else NY - 1
        return jnp.where(
            edge,
            pltpu.roll(view.tile(f, x, 1 - ty, tz), shift, 0),
            pltpu.roll(view.tile(f, x, ty, tz), shift, 0),
        )
    edge = lax.broadcasted_iota(jnp.int32, TILE, 1) == (0 if step < 0 else NZ - 1)
    return jnp.where(edge, view.tile(f, x, ty, 1 - tz, -step), view.tile(f, x, ty, tz, -step))


def two_sum(a, b):
    s = a + b
    t = s - a
    return s, (a - (s - t)) + (b - t)


def add_pair(a, b):
    s, e = two_sum(a[0], b[0])
    return s, e + (a[1] + b[1])


def halves(a):
    c = 4097.0 * a
    top = c - (c - a)
    return top, a - top


def product(a, b, a_halves, b_halves):
    (ah, al), (bh, bl) = a_halves, b_halves
    p = a * b
    return p, ((ah * bh - p) + ah * bl + al * bh) + al * bl


class Pair:
    def __init__(self, high, low):
        self.high, self.low = two_sum(high, low)
        self.halves = halves(self.high)

    def times(self, other):
        p, e = product(self.high, other.high, self.halves, other.halves)
        return p, e + (self.high * other.low + self.low * other.high)


def minimizer(high, low):
    size = KRYLOV + 1
    row = lax.broadcasted_iota(jnp.int32, TILE, 0)
    col = lax.broadcasted_iota(jnp.int32, TILE, 1)
    groups = (NY + 3 - 1, 2)
    assert groups[0] == size - 1

    def column(j, group):
        i = groups[group] - row
        mask = col == lax.shift_right_arithmetic(i * (i + 1), 1) + j
        return tuple(
            jnp.broadcast_to(jnp.sum(jnp.where(mask, v, 0.0), axis=1, keepdims=True), TILE)
            for v in (high, low)
        )

    def place(i):
        return (0, groups[0] - i) if i > groups[1] else (1, groups[1] - i)

    def entry(vectors, i):
        group, r = place(i)
        return tuple(jnp.broadcast_to(v[r : r + 1, :], TILE) for v in vectors[group])

    columns = [{g: column(j, g) for g in range(2) if g == 0 or j <= groups[1]} for j in range(size)]
    first = entry(columns[0], 0)
    right = {0: first, 1: first}
    factors, solved = [], []
    for k in range(size):
        pivot = Pair(*entry(columns[k], k))
        guess = 1.0 / pivot.high
        p, e = product(pivot.high, guess, pivot.halves, halves(guess))
        inverse = Pair(guess, guess * (((1.0 - p) - e) - pivot.low * guess))
        bk = Pair(*entry(right, k))
        solved.append(sum(bk.times(inverse)))
        live = [g for g in range(2) if (g == 0 and k < size - 1) or (g == 1 and k < groups[1])]
        factor = {g: Pair(*Pair(*columns[k][g]).times(inverse)) for g in live}
        factors.append({g: (factor[g].high, factor[g].low) for g in live})
        targets = [(columns[j], Pair(*entry(columns[k], j))) for j in range(k + 1, size)]
        for target, by in targets + [(right, bk)]:
            for g in live:
                if g in target:
                    p, e = factor[g].times(by)
                    s, t = two_sum(target[g][0], -p)
                    target[g] = s, target[g][1] + (t - e)
    z = [None] * size
    for k in range(size - 1, -1, -1):
        rest = solved[k]
        for i in range(size - 1, k, -1):
            rest = rest - entry(factors[k], i)[0] * z[i]
        z[k] = rest
    return z


def cycle_kernel(
    sizes,
    source_hbm, intra_hbm, extra_hbm, membrane_hbm,
    solution_ref, residual_ref, scale_ref,
    basis, coef, block, inverse,
    s_own, u_own, *refs,
):
    groups = [refs[10 * n : 10 * n + 10] for n in range(3)]
    gram_all, mine, parts, local_sem, sum_send, sum_recv = refs[30:]
    where = [lax.axis_index(a) for a in AXES]
    s_deep = s_own.at[pl.ds(0, MEMBRANE + 1)]
    cells, deep_cells, halo = (
        Halo(depth, (own, *group), where, sizes)
        for depth, own, group in zip((FIRST, DEEP, DEEP), (s_own, s_deep, u_own), groups)
    )

    deep_cells.gx = cells.gx

    def all_messages(h, plane_sets, row_sets):
        made = [h.edge(d) for d in CORNERS]
        for d in EDGES:
            if d[2]:
                made.append(h.edge(d))
            else:
                made += [h.corner_rows(d, *fields) for fields in row_sets]
        for d in FACES:
            if d[0]:
                made += [h.planes(d, *planes) for planes in plane_sets]
            elif d[1]:
                made.append(h.rows(d, slice(None), 0, h.depth))
            else:
                made.append(h.columns(d))
        return made

    first_messages = all_messages(cells, [
        (pl.ds(0, 2), 0, FIRST), (pl.ds(2, 7), 0, FIRST - 1),
    ], [(pl.ds(0, 4), FIRST - 1), (pl.ds(4, 5), FIRST - 2)])
    deep_messages = all_messages(deep_cells, [
        (pl.ds(0, 2), FIRST, 1), (pl.ds(2, 5), FIRST - 1, 1),
    ], [(pl.ds(0, 4), DEEP - 1), (pl.ds(4, 3), DEEP - 2)])
    messages = all_messages(halo, [(slice(None), 0, DEEP)], [(slice(None), DEEP - 1)])

    loads = [
        pltpu.make_async_copy(ref.at[axis], s_own.at[2 * axis + s], local_sem.at[2 * axis + s])
        for axis in range(3) for s, ref in enumerate((intra_hbm, extra_hbm))
    ] + [
        pltpu.make_async_copy(membrane_hbm, s_own.at[6], local_sem.at[6]),
        pltpu.make_async_copy(source_hbm, s_own.at[pl.ds(7, 2)], local_sem.at[7]),
    ]
    for c in loads:
        c.start()
    def clear(h):
        for ref in (h.gx, h.gy, h.gz, h.gxy, h.gxz, h.gyz, h.gxyz):
            if h is not deep_cells or ref is not h.gx:
                ref[...] = jnp.zeros_like(ref)

    clear(cells)
    clear(deep_cells)

    barrier = pltpu.get_barrier_semaphore()
    expected = 0
    for d in DIRECTIONS:
        there = cells.exists(d)
        expected = expected + jnp.where(there, 1, 0)

        @pl.when(there)
        def _(d=d):
            pl.semaphore_signal(
                barrier, inc=1,
                device_id=toward(where, sizes, d),
                device_id_type=MESH,
            )
    for d in range(3):
        for far in range(5, sizes[d]):
            for step in (-far, far):
                there = where[d] >= far if step < 0 else where[d] < sizes[d] - far
                expected = expected + jnp.where(there, 1, 0)

                @pl.when(there)
                def _(d=d, step=step):
                    pl.semaphore_signal(
                        barrier, inc=1, device_id={AXES[d]: lax.rem(where[d] + step + sizes[d], sizes[d])}, device_id_type=MESH
                    )
    gram_all[...] = jnp.zeros_like(gram_all)
    clear(halo)
    for k in range(1, KRYLOV + 1):
        basis[k] = jnp.zeros_like(basis.at[k])
    for c in loads:
        c.wait()
    cells.fill_pack([s_own[f, x] for f in range(FIELDS) for x in range(NX)])
    pl.semaphore_wait(barrier, expected)

    cells.start(0, first_messages)
    deep_cells.fill_pack([s_own[f, x] for f in range(MEMBRANE + 1) for x in range(NX)])
    deep_cells.start(0, deep_messages)

    def coefficients(view, cells_at):
        for t in cells_at:
            n = PLACE[t]
            diagonals = []
            for s in range(2):
                total = None
                for axis in range(3):
                    here = view.tile(2 * axis + s, *t)
                    lower = 0.5 * (here + beside(view, 2 * axis + s, t, axis, -1))
                    upper = 0.5 * (here + beside(view, 2 * axis + s, t, axis, 1))
                    coef[s, n, 2 * axis] = lower
                    coef[s, n, 2 * axis + 1] = upper
                    total = upper + lower if total is None else total + upper + lower
                diagonals.append(total)
            di, de, m = diagonals[0], diagonals[1], view.tile(MEMBRANE, *t)
            det = m * di + m * de + di * de
            inside = m > 0.0
            over = jnp.where(inside, 1.0 / jnp.where(inside, det, 1.0), 0.0)
            block[n, 0] = de * over
            block[n, 1] = m * over
            block[n, 2] = -di * over
            block[n, 3] = (m + di) * over
            if t in own:
                inverse[t[0]] = (di + de) * over

    own = [(x, OWN, OWN) for x in range(NX)]
    def solved(t, a, b):
        n = PLACE[t]
        return block[n, 0] * a + block[n, 1] * b, block[n, 2] * a + block[n, 3] * b

    def apply(view, t):
        n = PLACE[t]
        off = []
        for s in range(2):
            total = None
            for axis in range(3):
                for side, step in enumerate((-1, 1)):
                    term = coef[s, n, 2 * axis + side] * beside(view, s, t, axis, step)
                    total = term if total is None else total + term
            off.append(total)
        return off[0], off[0] + off[1]

    def load(k):
        return [[basis[k, s, x] for x in range(NX)] for s in range(2)]

    def keep(k, v):
        for s in range(2):
            for x in range(NX):
                basis[k, s, x] = v[s][x]

    def stage(h, v):
        values = [[None] * NX for _ in range(2)]
        for x in range(NX):
            values[0][x], values[1][x] = solved(own[x], v[0][x], v[1][x])
        for s in range(2):
            for x in range(NX):
                u_own[s, x] = values[s][x]
        h.fill_pack(values[0] + values[1])

    def gram_row(k):
        at, first = load(k), k * (k + 1) // 2
        for i in range(k + 1):
            total = None
            for s in range(2):
                for x in range(NX):
                    term = at[s][x] * basis[i, s, x]
                    total = term if total is None else total + term
            gram_all[pl.ds(first + i, 1), :] = jnp.sum(total, axis=0, keepdims=True)

    def powers(view, depth):
        made = []
        for reach in range(depth - 1, -1, -1):
            now = {t: apply(view, t) for t in tiles(reach)}
            made.append([[now[t][s] for t in own] for s in range(2)])
            if reach:
                view = solved_at(now)
        return made

    def solved_at(pairs):
        then = {t: solved(t, *pair) for t, pair in pairs.items()}
        return Values([{t: then[t][s] for t in then} for s in range(2)])

    def combine(f, *vs):
        return [[f(*(v[s][x] for v in vs)) for x in range(NX)] for s in range(2)]

    def advance(k, view, depth):
        here = load(k)
        made = powers(view, depth)
        terms = [
            made[0],
            combine(lambda b, a: 2.0 * b - a, made[1], here),
        ]
        if depth > 2:
            terms.append(combine(lambda b, a: 4.0 * b - 3.0 * a, made[2], made[0]))
            terms.append(combine(lambda b, a, r: 8.0 * b - 8.0 * a + r, made[3], made[1], here))
        if k == 0:
            return terms
        return [
            combine(lambda t, p: 2.0 * t - p, t, load(abs(k - 1 - j))) for j, t in enumerate(terms)
        ]

    def extend(k, made):
        for j, v in enumerate(made):
            keep(k + 1 + j, v)
        for j in range(len(made)):
            gram_row(k + 1 + j)

    keep(0, [[s_own[SOURCE + s, x] for x in range(NX)] for s in range(2)])
    gram_row(0)
    cells.sent(0, first_messages)
    cells.arrived(0, first_messages)
    view = cells.view(0)
    coefficients(view, tiles(FIRST - 1))
    start = {t: [view.tile(SOURCE + s, *t) for s in range(2)] for t in tiles(FIRST - 1)}
    made = advance(0, solved_at(start), FIRST - 1)
    stage(halo, made[-1])
    halo.start(0, messages)
    extend(0, made)
    deep_cells.sent(0, deep_messages)
    deep_cells.arrived(0, deep_messages)
    complete = [(x, OWN, OWN) for x in range(1 - FIRST, NX + FIRST - 1)]
    coefficients(deep_cells.view(0), [t for t in TILES if t not in complete])
    for slot, k in enumerate((2, 6)):
        halo.sent(slot, messages)
        halo.arrived(slot, messages)
        made = advance(k, halo.view(slot), DEEP)
        if slot == 0:
            stage(halo, made[-1])
            halo.start(1, messages)
        extend(k, made)

    ones = jnp.ones(TILE, jnp.bfloat16)
    left, totals = gram_all[...], []
    for _ in range(3):
        piece = left.astype(jnp.bfloat16)
        left = left - piece.astype(jnp.float32)
        totals.append(lax.dot_general(
            ones, piece, (((1,), (1,)), ((), ())), preferred_element_type=jnp.float32
        )[0:1, :])
    high, low = two_sum(totals[0], totals[1])
    low = low + totals[2]
    for n, d in enumerate((2, 1, 0)):
        size = sizes[d]
        mine[n, 0:1, :] = high
        mine[n, 1:2, :] = low
        parts[n, where[d], 0:1, :] = high
        parts[n, where[d], 1:2, :] = low

        def copy(j, slot, other):
            return pltpu.make_async_remote_copy(
                src_ref=mine.at[n, pl.ds(0, 2), :], dst_ref=parts.at[n, slot, pl.ds(0, 2), :],
                send_sem=sum_send.at[n, j], recv_sem=sum_recv.at[n, slot],
                device_id={AXES[d]: other}, device_id_type=MESH,
            )

        others = [(j, lax.rem(where[d] + j, size)) for j in range(1, size)]
        for j, other in others:
            copy(j, where[d], other).start()
        for j, other in others:
            copy(j, other, other).wait_recv()
        for j, other in others:
            copy(j, where[d], other).wait_send()
        terms = [(parts[n, j, 0:1, :], parts[n, j, 1:2, :]) for j in range(size)]
        while len(terms) > 1:
            terms = [add_pair(terms[i], terms[i + 1]) for i in range(0, len(terms), 2)]
        high, low = two_sum(*terms[0])

    z = minimizer(jnp.broadcast_to(high, TILE), jnp.broadcast_to(low, TILE))
    size = KRYLOV + 1
    total = z[0]
    for k in range(1, size):
        total = total + z[k]
    scale_ref[...] = 1.0 / total
    rho = z
    slope = [None] * size
    running = jnp.zeros(TILE, jnp.float32)
    weighted = jnp.zeros(TILE, jnp.float32)
    for j in range(KRYLOV - 1, -1, -1):
        running = running + rho[j + 1]
        weighted = weighted + running
        slope[j] = weighted
    coeffs = [slope[0]] + [2.0 * slope[j] for j in range(1, KRYLOV)]

    for x in range(NX):
        combined = []
        for s in range(2):
            vectors = [basis[k, s, x] for k in range(size)]
            r = rho[0] * vectors[0]
            c = coeffs[0] * vectors[0]
            for k in range(1, size):
                r = r + rho[k] * vectors[k]
                if k < KRYLOV:
                    c = c + coeffs[k] * vectors[k]
            residual_ref[s, x] = r
            combined.append(c)
        n = PLACE[own[x]]
        solution_ref[0, x] = inverse[x] * combined[0] + block[n, 2] * combined[1]
        solution_ref[1, x] = block[n, 2] * combined[0] + block[n, 3] * combined[1]


def halo_scratch(depth, fields, slots, count):
    vm = lambda *s: pltpu.VMEM(s, jnp.float32)
    dma = pltpu.SemaphoreType.DMA
    packs = -(-fields * NX // (NZ // (2 * depth)))
    return [
        vm(packs, *TILE),
        vm(slots, 2, fields, DEEP, *TILE), vm(slots, fields, NX, *TILE),
        vm(slots, 2, packs, *TILE), vm(slots, 2, fields, depth - 1, *TILE),
        vm(slots, 2, 2, packs, *TILE), vm(slots, 2, packs, *TILE), vm(slots, 2, 2, packs, *TILE),
        dma((count,)), dma((slots, count)),
    ]


def body(source, sigma_intra, sigma_extra, membrane):
    sizes = tuple(lax.axis_size(a) for a in AXES)
    f32 = jnp.float32
    vm = lambda *s: pltpu.VMEM(s, f32)
    dma = pltpu.SemaphoreType.DMA
    count = len(TILES)
    unscaled, remainder, scale = pl.pallas_call(
        functools.partial(cycle_kernel, sizes),
        out_shape=(vm(*source.shape), vm(*source.shape), vm(*TILE)),
        in_specs=[pl.BlockSpec(memory_space=pl.ANY)] * 4,
        out_specs=(pl.BlockSpec(memory_space=pltpu.VMEM),) * 3,
        scratch_shapes=[
            vm(KRYLOV + 1, 2, NX, *TILE), vm(2, count, 6, *TILE), vm(count, 4, *TILE), vm(NX, *TILE),
            vm(FIELDS, NX, *TILE), vm(2, NX, *TILE),
            *halo_scratch(FIRST, FIELDS, 1, 32), *halo_scratch(DEEP, MEMBRANE + 1, 1, 32),
            *halo_scratch(DEEP, 2, 2, 26),
            vm(128, NZ), vm(3, *TILE), vm(3, 8, *TILE),
            dma((8,)), dma((3, 8)), dma((3, 8)),
        ],
        compiler_params=pltpu.CompilerParams(collective_id=0, has_side_effects=True),
    )(source, sigma_intra, sigma_extra, membrane)
    return unscaled * scale, remainder * scale


def solution(mesh):
    return jax.shard_map(
        body,
        mesh=mesh,
        in_specs=(
            P(None, "gx", "gy", "gz"),
            P(None, "gx", "gy", "gz"),
            P(None, "gx", "gy", "gz"),
            P("gx", "gy", "gz"),
        ),
        out_specs=(P(None, "gx", "gy", "gz"), P(None, "gx", "gy", "gz")),
        check_vma=False,
    )
```
